32 devices in a mesh: dp: 4 (over z), fsdp: 8 (over y, x, core).
Axes of the slice: x: 2, y: 2, z: 4, core: 2. Of those that a mesh axis runs over, the one named last changes fastest.
Arguments:
- hidden: bfloat16 [65536, 1024], P(('dp', 'fsdp')), may hold values from -6 to 6
- cotangent: bfloat16 [65536, 1024], P(('dp', 'fsdp')), may hold values from -6 to 6
- route_pos: int32 [32, 256], P(('dp', 'fsdp')), may hold values from 0 to 2047, as said below
- route_doc: int32 [32, 256], P(('dp', 'fsdp')), may hold values from 0 to 2, as said below
- w_qkv: bfloat16 [1024, 3072], P('fsdp'), may hold values from -0.1875 to 0.1875
- w_out: bfloat16 [1024, 1024], P('fsdp'), may hold values from -0.75 to 0.75
- w_up: bfloat16 [1024, 4096], P('fsdp'), may hold values from -0.1875 to 0.1875
- w_down: bfloat16 [4096, 1024], P('fsdp'), may hold values from -0.09375 to 0.09375
- router: float32 [1024], replicated, may hold values from -0.1875 to 0.1875
- gain_one: float32 [1024], replicated, may hold values from 0.5 to 1.5
- gain_two: float32 [1024], replicated, may hold values from 0.5 to 1.5
Outputs:
- output: bfloat16 [65536, 1024], P(('dp', 'fsdp'))
- grad_hidden: bfloat16 [65536, 1024], P(('dp', 'fsdp'))
- grad_qkv: float32 [1024, 3072], P('fsdp')
- grad_out: float32 [1024, 1024], P('fsdp')
- grad_up: float32 [1024, 4096], P('fsdp')
- grad_down: float32 [4096, 1024], P('fsdp')
- grad_router: float32 [1024], replicated
- grad_gain_one: float32 [1024], replicated
- grad_gain_two: float32 [1024], replicated
The draws below stay inside these ranges and needn't reach their ends.
Inputs may be any that keep to these rules, and one draw needn't show every extreme that they name: `route_pos`: A buffer holds one sequence of 1024 tokens, one of 2048, or two of 1024, each starting at a multiple of 1024; a sequence of L tokens has L / 8 routed slots. Slots of a buffer are distinct and ascending, and the buffer's last slot is routed. `route_doc`: 0 and 1 name the sequences of a buffer; 2 marks an empty slot. In every draw some buffer has all 256 slots live and some has half of them empty.
All inputs are finite; a program needn't handle non-finite values.
Results may differ from the reference program's by a relative error of at most 0.011.
Values may be sent and summed in bfloat16 or wider, within the bound.
A program may use at most 192 MiB of HBM per device.

```python
import jax
import jax.numpy as jnp
from jax import lax

D = 1024
HEADS = 16
HEAD = 64
FF = 4096
SEQ_UNIT = 1024
TOK_DEV = 2048
SHARDS = 32
TOKENS = 65536


def layout(key):
    base_key = jax.random.fold_in(key, 7)
    kind_key, force_key, other_key, perm_key = jax.random.split(base_key, 4)
    kind_draw = jax.random.randint(kind_key, (SHARDS,), 0, 3)
    forced = jax.random.randint(force_key, (), 0, SHARDS)
    forced_two = (forced + 1 + jax.random.randint(other_key, (), 0, SHARDS - 1)) % SHARDS
    device_ids = jnp.arange(SHARDS)
    kind_draw = jnp.where(device_ids == forced, 2, kind_draw)
    kind_draw = jnp.where(device_ids == forced_two, 0, kind_draw)

    def one_device(device_key, layout_kind):
        shuffled = jax.random.permutation(device_key, TOK_DEV).astype(jnp.int32)
        shuffled = shuffled.at[TOK_DEV - 1].set(-1)
        unit_rows = shuffled.reshape(2, SEQ_UNIT)
        per_unit = jnp.argsort(unit_rows, axis=1)[:, :SEQ_UNIT // 8] + (jnp.arange(2) * SEQ_UNIT)[:, None]
        per_unit = per_unit.reshape(-1).astype(jnp.int32)
        whole_seq = jnp.argsort(shuffled)[:TOK_DEV // 8].astype(jnp.int32)
        chosen = jnp.sort(jnp.where(layout_kind == 1, whole_seq, per_unit)).astype(jnp.int32)
        unit_index = chosen // SEQ_UNIT
        doc_ids = jnp.where(layout_kind == 2, unit_index, jnp.where(layout_kind == 1, 0, 2 * unit_index))
        return (chosen, doc_ids.astype(jnp.int32))
    device_keys = jax.random.split(perm_key, SHARDS)
    return jax.vmap(one_device)(device_keys, kind_draw)


def draw_route_pos(key, part):
    return layout(key)[0]


def draw_route_doc(key, part):
    return layout(key)[1]


def draw_cotangent(key, part):
    base = jnp.clip(jax.random.normal(key, (TOKENS, D), jnp.float32), -4.0, 4.0)
    block_index = (jnp.arange(TOKENS) // TOK_DEV).astype(jnp.float32)
    factor = 0.5 + block_index / max(SHARDS - 1, 1)
    return (base * factor[:, None]).astype(jnp.bfloat16)


def shard_levels(stream_key, shape, cuts, smallest, top_value):
    gain, own = 1.0, jax.random.fold_in(stream_key, 6)
    for position, blocks in cuts:
        draws = jnp.exp(jax.random.uniform(jax.random.fold_in(own, position), (blocks,), jnp.float32, smallest / len(cuts), top_value / len(cuts)))
        gain = gain * jnp.repeat(draws, shape[position] // blocks).reshape([-1 if axis == position else 1 for axis in range(len(shape))])
    return gain


def gaussian(key, extent, scale, reach, cuts=(), kind=jnp.bfloat16):
    array = scale * jax.random.normal(key, extent, jnp.float32)
    if cuts:
        array = array * shard_levels(key, extent, cuts, -0.22, 0.18)
    return jnp.clip(array, -reach, reach).astype(kind)


def setup_inputs(seed: int = 0) -> dict:
    arg_keys = jax.random.split(jax.random.key(seed), 12)
    hidden = gaussian(arg_keys[0], (TOKENS, D), 1.0, 6.0, ((0, 32),))
    cotangent = draw_cotangent(jax.random.fold_in(arg_keys[11], 71), 0)
    route_pos = draw_route_pos(jax.random.fold_in(arg_keys[11], 71), 0)
    route_doc = draw_route_doc(jax.random.fold_in(arg_keys[11], 71), 0)
    w_qkv = gaussian(arg_keys[4], (D, 3 * D), D ** -0.5, 0.1875, ((0, 8),))
    w_out = gaussian(arg_keys[5], (D, D), (D // 16) ** -0.5, 0.75, ((0, 8),))
    w_up = gaussian(arg_keys[6], (D, FF), D ** -0.5, 0.1875, ((0, 8),))
    w_down = gaussian(arg_keys[7], (FF, D), FF ** -0.5, 0.09375, ((0, 8),))
    router = gaussian(arg_keys[8], (D,), D ** -0.5, 0.1875, (), jnp.float32)
    gain_one = jnp.clip(1.0 + 0.1 * jax.random.normal(arg_keys[9], (D,), jnp.float32), 0.5, 1.5)
    gain_two = jnp.clip(1.0 + 0.1 * jax.random.normal(arg_keys[10], (D,), jnp.float32), 0.5, 1.5)
    return {"hidden": hidden, "cotangent": cotangent, "route_pos": route_pos, "route_doc": route_doc, "w_qkv": w_qkv, "w_out": w_out, "w_up": w_up, "w_down": w_down, "router": router, "gain_one": gain_one, "gain_two": gain_two}


EPS = 1e-06

@jax.custom_vjp
def low(v):
    return lax.optimization_barrier(v.astype(jnp.bfloat16)).astype(jnp.float32)

@jax.custom_vjp
def low_back(v):
    return v

def low_keep(v):
    return (low(v), None)

def low_pass(kept, grad):
    return (grad,)

def back_keep(v):
    return (v, None)

def back_low(kept, grad):
    return (low(grad),)
low.defvjp(low_keep, low_pass)
low_back.defvjp(back_keep, back_low)

def matmul_hi(left, right):
    return jnp.dot(left, right, precision=lax.Precision.HIGHEST)

def rms_scale(values, gain_vec):
    return values * lax.rsqrt(lax.optimization_barrier(jnp.mean(values * values, axis=-1, keepdims=True)) + EPS) * gain_vec

def branch(routed, positions, documents, qkv_w, out_w, up_w, down_w, router_w, gain_a, gain_b):
    row_count = routed.shape[0]
    router_out = matmul_hi(routed, router_w)
    normed_in = low(rms_scale(routed, gain_a))
    packed = low(low_back(matmul_hi(normed_in, qkv_w)))
    query_heads = packed[:, :D].reshape(row_count, HEADS, HEAD)
    key_heads = packed[:, D:2 * D].reshape(row_count, HEADS, HEAD)
    value_heads = packed[:, 2 * D:].reshape(row_count, HEADS, HEAD)
    scores = jnp.einsum('qhd,khd->hqk', query_heads, key_heads, precision=lax.Precision.HIGHEST) * 0.125
    allowed = (documents[:, None] == documents[None, :]) & (positions[None, :] <= positions[:, None])
    scores = low_back(jnp.where(allowed[None], scores, -1000000000.0))
    prob_rows = low(jax.nn.softmax(scores, axis=-1))
    attended = jnp.einsum('hqk,khd->qhd', prob_rows, value_heads, precision=lax.Precision.HIGHEST)
    attended = low(low_back(attended.reshape(row_count, D)))
    attn_out = low_back(matmul_hi(attended, out_w))
    middle = routed + attn_out
    normed_mid = low(rms_scale(middle, gain_b))
    up_in = low_back(matmul_hi(normed_mid, up_w))
    activated = low(jax.nn.gelu(up_in))
    mlp_out = low_back(matmul_hi(activated, down_w))
    live_mask = (documents < 2).astype(routed.dtype)
    return (live_mask * router_out)[:, None] * (attn_out + mlp_out)

def reference(hidden, cotangent, route_pos, route_doc, w_qkv, w_out, w_up, w_down, router, gain_one, gain_two):
    weights = (w_qkv.astype(jnp.float32), w_out.astype(jnp.float32), w_up.astype(jnp.float32), w_down.astype(jnp.float32), router, gain_one, gain_two)

    def device_step(running, blocks):
        tokens, grad_tokens, positions, documents = blocks

        def layer(token_rows, qkv_w, out_w, up_w, down_w, router_w, gain_a, gain_b):
            added = branch(token_rows[positions], positions, documents, qkv_w, out_w, up_w, down_w, router_w, gain_a, gain_b)
            return token_rows.at[positions].add(added)
        result, pull = jax.vjp(layer, tokens.astype(jnp.float32), *weights)
        grads = pull(grad_tokens.astype(jnp.float32))
        running = tuple((sofar + addend for sofar, addend in zip(running, grads[1:])))
        return (running, (result.astype(jnp.bfloat16), grads[0].astype(jnp.bfloat16)))
    start = tuple((jnp.zeros_like(weight) for weight in weights))
    blocks = (hidden.reshape(SHARDS, TOK_DEV, D), cotangent.reshape(SHARDS, TOK_DEV, D), route_pos, route_doc)
    running, (output, grad_hidden) = lax.scan(device_step, start, blocks)
    return (output.reshape(TOKENS, D), grad_hidden.reshape(TOKENS, D), running[0], running[1], running[2], running[3], running[4], running[5], running[6])
```

```python
import jax
import jax.numpy as jnp
from jax import lax
from jax.sharding import PartitionSpec as P

D = 1024
HEADS = 16
HEAD = 64


EPS = 1e-06


def rms_scale(values, gain_vec):
    return values * lax.rsqrt(jnp.mean(values * values, axis=-1, keepdims=True) + EPS) * gain_vec


def forward(tokens, positions, documents, weights, router, gain_one, gain_two):
    full_qkv, full_out, full_up, full_down = weights
    routed = tokens[positions].astype(jnp.float32)
    row_count = routed.shape[0]
    router_out = jnp.dot(routed, router, precision=lax.Precision.HIGHEST)
    normed_in = rms_scale(routed, gain_one).astype(jnp.bfloat16)
    packed = jnp.dot(normed_in, full_qkv, preferred_element_type=jnp.float32).astype(jnp.bfloat16)
    heads = packed.reshape(row_count, 3, HEADS, HEAD)
    allowed = (documents[:, None] == documents[None, :]) & (
        positions[None, :] <= positions[:, None]
    )
    scores = (
        jnp.einsum("qhd,khd->hqk", heads[:, 0], heads[:, 1], preferred_element_type=jnp.float32)
        * 0.125
    )
    scores = jnp.where(allowed[None], scores, -1000000000.0)
    row_max = jnp.max(scores, axis=-1, keepdims=True)
    log_total = row_max + jnp.log(jnp.sum(jnp.exp(scores - row_max), axis=-1, keepdims=True))
    prob_rows = jnp.exp(scores - log_total)
    prob_low = prob_rows.astype(jnp.bfloat16)
    attended = jnp.einsum("hqk,khd->qhd", prob_low, heads[:, 2], preferred_element_type=jnp.float32)
    attended = attended.reshape(row_count, D).astype(jnp.bfloat16)
    attn_out = jnp.dot(attended, full_out, preferred_element_type=jnp.float32)
    middle = routed + attn_out
    normed_mid = rms_scale(middle, gain_two).astype(jnp.bfloat16)
    up_in = jnp.dot(normed_mid, full_up, preferred_element_type=jnp.float32)
    activated = jax.nn.gelu(up_in).astype(jnp.bfloat16)
    mlp_out = jnp.dot(activated, full_down, preferred_element_type=jnp.float32)
    return (
        routed,
        router_out,
        normed_in,
        heads,
        prob_rows,
        prob_low,
        attended,
        attn_out,
        middle,
        normed_mid,
        up_in,
        activated,
        mlp_out,
    )


def per_device(
    hidden, cotangent, route_pos, route_doc, w_qkv, w_out, w_up, w_down, router, gain_one, gain_two
):
    positions = route_pos[0]
    documents = route_doc[0]
    live_mask = (documents < 2).astype(jnp.float32)[:, None]
    gathered = (
        lax.all_gather(w_qkv, "fsdp", axis=0, tiled=True),
        lax.all_gather(w_out, "fsdp", axis=0, tiled=True),
        lax.all_gather(w_up, "fsdp", axis=0, tiled=True),
        lax.all_gather(w_down, "fsdp", axis=0, tiled=True),
    )
    state = forward(hidden, positions, documents, gathered, router, gain_one, gain_two)
    attn_first = state[7]
    mlp_first = state[12]
    added = live_mask * state[1][:, None] * (attn_first + mlp_first)
    output = hidden.astype(jnp.float32).at[positions].add(added).astype(jnp.bfloat16)
    weights = (
        lax.all_gather(w_qkv, "fsdp", axis=0, tiled=True),
        lax.all_gather(w_out, "fsdp", axis=0, tiled=True),
        lax.all_gather(w_up, "fsdp", axis=0, tiled=True),
        lax.all_gather(w_down, "fsdp", axis=0, tiled=True),
    )
    state = forward(hidden, positions, documents, weights, router, gain_one, gain_two)
    full_qkv, full_out, full_up, full_down = weights
    (
        routed,
        router_out,
        normed_in,
        heads,
        prob_rows,
        prob_low,
        attended,
        attn_out,
        middle,
        normed_mid,
        up_in,
        activated,
        mlp_out,
    ) = state
    row_count = routed.shape[0]
    branch_out = attn_out + mlp_out
    grad_add = live_mask * cotangent[positions].astype(jnp.float32)
    grad_branch = grad_add * router_out[:, None]
    grad_score = jnp.sum(grad_add * branch_out, axis=-1)
    grad_mlp = grad_branch.astype(jnp.bfloat16)
    grad_down = jnp.dot(activated.T, grad_mlp, preferred_element_type=jnp.float32)
    grad_act = jnp.dot(grad_mlp, full_down.T, preferred_element_type=jnp.float32)
    _, gelu_pull = jax.vjp(jax.nn.gelu, up_in)
    grad_up_in = gelu_pull(grad_act)[0].astype(jnp.bfloat16)
    grad_up = jnp.dot(normed_mid.T, grad_up_in, preferred_element_type=jnp.float32)
    grad_norm_mid = jnp.dot(grad_up_in, full_up.T, preferred_element_type=jnp.float32)
    _, second_pull = jax.vjp(rms_scale, middle, gain_two)
    grad_middle, grad_gain_two = second_pull(grad_norm_mid)
    grad_attn = (grad_branch + grad_middle).astype(jnp.bfloat16)
    grad_out = jnp.dot(attended.T, grad_attn, preferred_element_type=jnp.float32)
    grad_attended = jnp.dot(grad_attn, full_out.T, preferred_element_type=jnp.float32).astype(
        jnp.bfloat16
    )
    grad_attended = grad_attended.reshape(row_count, HEADS, HEAD)
    grad_prob = jnp.einsum(
        "qhd,khd->hqk", grad_attended, heads[:, 2], preferred_element_type=jnp.float32
    )
    grad_value = jnp.einsum(
        "hqk,qhd->khd", prob_low, grad_attended, preferred_element_type=jnp.float32
    )
    row_dot = jnp.sum(grad_prob * prob_rows, axis=-1, keepdims=True)
    grad_scores = (prob_rows * (grad_prob - row_dot)).astype(jnp.bfloat16)
    grad_query = (
        jnp.einsum("hqk,khd->qhd", grad_scores, heads[:, 1], preferred_element_type=jnp.float32)
        * 0.125
    )
    grad_key = (
        jnp.einsum("hqk,qhd->khd", grad_scores, heads[:, 0], preferred_element_type=jnp.float32)
        * 0.125
    )
    grad_packed = jnp.stack([grad_query, grad_key, grad_value], axis=1).reshape(row_count, 3 * D)
    grad_packed = grad_packed.astype(jnp.bfloat16)
    grad_qkv = jnp.dot(normed_in.T, grad_packed, preferred_element_type=jnp.float32)
    grad_norm_in = jnp.dot(grad_packed, full_qkv.T, preferred_element_type=jnp.float32)
    _, first_pull = jax.vjp(rms_scale, routed, gain_one)
    grad_routed, grad_gain_one = first_pull(grad_norm_in)
    grad_routed = grad_routed + grad_middle + grad_score[:, None] * router[None, :]
    grad_router = jnp.dot(grad_score, routed, precision=lax.Precision.HIGHEST)
    grad_hidden = cotangent.astype(jnp.float32).at[positions].add(grad_routed).astype(jnp.bfloat16)
    shard_sums = (
        lax.psum_scatter(grad_qkv.astype(jnp.bfloat16), "fsdp", scatter_dimension=0, tiled=True),
        lax.psum_scatter(grad_out.astype(jnp.bfloat16), "fsdp", scatter_dimension=0, tiled=True),
        lax.psum_scatter(grad_up.astype(jnp.bfloat16), "fsdp", scatter_dimension=0, tiled=True),
        lax.psum_scatter(grad_down.astype(jnp.bfloat16), "fsdp", scatter_dimension=0, tiled=True),
    )
    final_sums = lax.psum((shard_sums[0], shard_sums[1], shard_sums[2], shard_sums[3]), "dp")
    small_sums = lax.psum((grad_router, grad_gain_one, grad_gain_two), ("dp", "fsdp"))
    return (
        output,
        grad_hidden,
        final_sums[0].astype(jnp.float32),
        final_sums[1].astype(jnp.float32),
        final_sums[2].astype(jnp.float32),
        final_sums[3].astype(jnp.float32),
        small_sums[0],
        small_sums[1],
        small_sums[2],
    )


def solution(mesh):
    return jax.shard_map(
        per_device,
        mesh=mesh,
        in_specs=(
            P(("dp", "fsdp"), None),
            P(("dp", "fsdp"), None),
            P(("dp", "fsdp"), None),
            P(("dp", "fsdp"), None),
            P("fsdp", None),
            P("fsdp", None),
            P("fsdp", None),
            P("fsdp", None),
            P(),
            P(),
            P(),
        ),
        out_specs=(
            P(("dp", "fsdp"), None),
            P(("dp", "fsdp"), None),
            P("fsdp", None),
            P("fsdp", None),
            P("fsdp", None),
            P("fsdp", None),
            P(),
            P(),
            P(),
        ),
        check_vma=False,
    )
```

```python
import functools

import jax
import jax.numpy as jnp
from jax import lax
from jax.experimental import pallas as pl
from jax.experimental.pallas import tpu as pltpu
from jax.sharding import PartitionSpec as P

D = 1024
HEADS = 16
HEAD = 64


EPS = 1e-06


def rms_scale(values, gain_vec):
    return values * lax.rsqrt(jnp.mean(values * values, axis=-1, keepdims=True) + EPS) * gain_vec


def forward(tokens, positions, documents, weights, router, gain_one, gain_two):
    full_qkv, full_out, full_up, full_down = weights
    routed = tokens[positions].astype(jnp.float32)
    row_count = routed.shape[0]
    router_out = jnp.dot(routed, router, precision=lax.Precision.HIGHEST)
    normed_in = rms_scale(routed, gain_one).astype(jnp.bfloat16)
    packed = jnp.dot(normed_in, full_qkv, preferred_element_type=jnp.float32).astype(jnp.bfloat16)
    heads = packed.reshape(row_count, 3, HEADS, HEAD)
    allowed = (documents[:, None] == documents[None, :]) & (
        positions[None, :] <= positions[:, None]
    )
    scores = (
        jnp.einsum("qhd,khd->hqk", heads[:, 0], heads[:, 1], preferred_element_type=jnp.float32)
        * 0.125
    )
    scores = jnp.where(allowed[None], scores, -1000000000.0)
    row_max = jnp.max(scores, axis=-1, keepdims=True)
    log_total = row_max + jnp.log(jnp.sum(jnp.exp(scores - row_max), axis=-1, keepdims=True))
    prob_rows = jnp.exp(scores - log_total)
    prob_low = prob_rows.astype(jnp.bfloat16)
    attended = jnp.einsum("hqk,khd->qhd", prob_low, heads[:, 2], preferred_element_type=jnp.float32)
    attended = attended.reshape(row_count, D).astype(jnp.bfloat16)
    attn_out = jnp.dot(attended, full_out, preferred_element_type=jnp.float32)
    middle = routed + attn_out
    normed_mid = rms_scale(middle, gain_two).astype(jnp.bfloat16)
    up_in = jnp.dot(normed_mid, full_up, preferred_element_type=jnp.float32)
    activated = jax.nn.gelu(up_in).astype(jnp.bfloat16)
    mlp_out = jnp.dot(activated, full_down, preferred_element_type=jnp.float32)
    return (
        routed,
        router_out,
        normed_in,
        heads,
        prob_rows,
        prob_low,
        attended,
        attn_out,
        middle,
        normed_mid,
        up_in,
        activated,
        mlp_out,
    )


def general_device(
    hidden, cotangent, route_pos, route_doc, w_qkv, w_out, w_up, w_down, router, gain_one, gain_two
):
    positions = route_pos[0]
    documents = route_doc[0]
    live_mask = (documents < 2).astype(jnp.float32)[:, None]
    gathered = (
        lax.all_gather(w_qkv, "fsdp", axis=0, tiled=True),
        lax.all_gather(w_out, "fsdp", axis=0, tiled=True),
        lax.all_gather(w_up, "fsdp", axis=0, tiled=True),
        lax.all_gather(w_down, "fsdp", axis=0, tiled=True),
    )
    state = forward(hidden, positions, documents, gathered, router, gain_one, gain_two)
    attn_first = state[7]
    mlp_first = state[12]
    added = live_mask * state[1][:, None] * (attn_first + mlp_first)
    output = hidden.astype(jnp.float32).at[positions].add(added).astype(jnp.bfloat16)
    weights = (
        lax.all_gather(w_qkv, "fsdp", axis=0, tiled=True),
        lax.all_gather(w_out, "fsdp", axis=0, tiled=True),
        lax.all_gather(w_up, "fsdp", axis=0, tiled=True),
        lax.all_gather(w_down, "fsdp", axis=0, tiled=True),
    )
    state = forward(hidden, positions, documents, weights, router, gain_one, gain_two)
    full_qkv, full_out, full_up, full_down = weights
    (
        routed,
        router_out,
        normed_in,
        heads,
        prob_rows,
        prob_low,
        attended,
        attn_out,
        middle,
        normed_mid,
        up_in,
        activated,
        mlp_out,
    ) = state
    row_count = routed.shape[0]
    branch_out = attn_out + mlp_out
    grad_add = live_mask * cotangent[positions].astype(jnp.float32)
    grad_branch = grad_add * router_out[:, None]
    grad_score = jnp.sum(grad_add * branch_out, axis=-1)
    grad_mlp = grad_branch.astype(jnp.bfloat16)
    grad_down = jnp.dot(activated.T, grad_mlp, preferred_element_type=jnp.float32)
    grad_act = jnp.dot(grad_mlp, full_down.T, preferred_element_type=jnp.float32)
    _, gelu_pull = jax.vjp(jax.nn.gelu, up_in)
    grad_up_in = gelu_pull(grad_act)[0].astype(jnp.bfloat16)
    grad_up = jnp.dot(normed_mid.T, grad_up_in, preferred_element_type=jnp.float32)
    grad_norm_mid = jnp.dot(grad_up_in, full_up.T, preferred_element_type=jnp.float32)
    _, second_pull = jax.vjp(rms_scale, middle, gain_two)
    grad_middle, grad_gain_two = second_pull(grad_norm_mid)
    grad_attn = (grad_branch + grad_middle).astype(jnp.bfloat16)
    grad_out = jnp.dot(attended.T, grad_attn, preferred_element_type=jnp.float32)
    grad_attended = jnp.dot(grad_attn, full_out.T, preferred_element_type=jnp.float32).astype(
        jnp.bfloat16
    )
    grad_attended = grad_attended.reshape(row_count, HEADS, HEAD)
    grad_prob = jnp.einsum(
        "qhd,khd->hqk", grad_attended, heads[:, 2], preferred_element_type=jnp.float32
    )
    grad_value = jnp.einsum(
        "hqk,qhd->khd", prob_low, grad_attended, preferred_element_type=jnp.float32
    )
    row_dot = jnp.sum(grad_prob * prob_rows, axis=-1, keepdims=True)
    grad_scores = (prob_rows * (grad_prob - row_dot)).astype(jnp.bfloat16)
    grad_query = (
        jnp.einsum("hqk,khd->qhd", grad_scores, heads[:, 1], preferred_element_type=jnp.float32)
        * 0.125
    )
    grad_key = (
        jnp.einsum("hqk,qhd->khd", grad_scores, heads[:, 0], preferred_element_type=jnp.float32)
        * 0.125
    )
    grad_packed = jnp.stack([grad_query, grad_key, grad_value], axis=1).reshape(row_count, 3 * D)
    grad_packed = grad_packed.astype(jnp.bfloat16)
    grad_qkv = jnp.dot(normed_in.T, grad_packed, preferred_element_type=jnp.float32)
    grad_norm_in = jnp.dot(grad_packed, full_qkv.T, preferred_element_type=jnp.float32)
    _, first_pull = jax.vjp(rms_scale, routed, gain_one)
    grad_routed, grad_gain_one = first_pull(grad_norm_in)
    grad_routed = grad_routed + grad_middle + grad_score[:, None] * router[None, :]
    grad_router = jnp.dot(grad_score, routed, precision=lax.Precision.HIGHEST)
    grad_hidden = cotangent.astype(jnp.float32).at[positions].add(grad_routed).astype(jnp.bfloat16)
    shard_sums = (
        lax.psum_scatter(grad_qkv.astype(jnp.bfloat16), "fsdp", scatter_dimension=0, tiled=True),
        lax.psum_scatter(grad_out.astype(jnp.bfloat16), "fsdp", scatter_dimension=0, tiled=True),
        lax.psum_scatter(grad_up.astype(jnp.bfloat16), "fsdp", scatter_dimension=0, tiled=True),
        lax.psum_scatter(grad_down.astype(jnp.bfloat16), "fsdp", scatter_dimension=0, tiled=True),
    )
    final_sums = lax.psum((shard_sums[0], shard_sums[1], shard_sums[2], shard_sums[3]), "dp")
    small_sums = lax.psum((grad_router, grad_gain_one, grad_gain_two), ("dp", "fsdp"))
    return (
        output,
        grad_hidden,
        final_sums[0].astype(jnp.float32),
        final_sums[1].astype(jnp.float32),
        final_sums[2].astype(jnp.float32),
        final_sums[3].astype(jnp.float32),
        small_sums[0],
        small_sums[1],
        small_sums[2],
    )


MESH = pl.DeviceIdType.MESH
ANY = pl.ANY


def flip(index, stride):
    return index + stride - 2 * stride * ((index // stride) % 2)


def places():
    z = lax.axis_index("dp")
    f = lax.axis_index("fsdp")
    return z, f, flip(f, 1), flip(f, 2), flip(f, 4), flip(flip(f, 2), 4)


def greet(peers):
    barrier = pltpu.get_barrier_semaphore()
    for peer in peers:
        pl.semaphore_signal(barrier, inc=1, device_id=peer, device_id_type=MESH)
    pl.semaphore_wait(barrier, len(peers))


GATHER_KINDS = 13


def gather_kernel(*refs):
    shards, fulls, kept = refs[0:4], refs[4:8], refs[8:12]
    kept_in, kept_out, send, recv = refs[12:16]
    z, f, core, along_x, along_y, across = places()
    pair = flip(z, 1)
    at_core, at_x, at_y, at_z = (z, core), (z, along_x), (z, along_y), (pair, f)
    greet((at_core, at_x, at_y, at_z))

    def rows_of(w, origin, start, size):
        rows = shards[w].shape[0]
        return pl.ds(pl.multiple_of(origin * rows + start, 16), size)

    def copy(w, kind, source, origin, start, size, peer):
        return pltpu.make_async_remote_copy(
            src_ref=source,
            dst_ref=fulls[w].at[rows_of(w, origin, start, size)],
            send_sem=send.at[w, kind],
            recv_sem=recv.at[w, kind],
            device_id=peer,
            device_id_type=MESH,
        )

    def own(w, kind, start, size, peer):
        source = shards[w].at[pl.ds(pl.multiple_of(start, 16), size)]
        return copy(w, kind, source, f, start, size, peer)

    def passed(w, kind, origin, start, size, peer):
        return copy(w, kind, fulls[w].at[rows_of(w, origin, start, size)], origin, start, size, peer)

    plan = []
    for w in range(4):
        rows = shards[w].shape[0]
        half = rows // 2
        even, odd = (z % 2) * half, (1 - z % 2) * half
        plan.append(
            [
                own(w, 0, even, half, at_x),
                own(w, 1, odd, half, at_y),
                own(w, 2, 0, rows, at_core),
                passed(w, 3, along_y, odd, half, at_x),
                passed(w, 4, along_x, even, half, at_y),
                passed(w, 5, along_x, even, half, at_z),
                passed(w, 6, along_y, odd, half, at_z),
                passed(w, 7, along_x, even, half, at_core),
                passed(w, 8, along_y, odd, half, at_core),
                passed(w, 9, across, odd, half, at_core),
                passed(w, 10, across, even, half, at_core),
                passed(w, 11, along_x, odd, half, at_core),
                passed(w, 12, along_y, even, half, at_core),
            ]
        )

    def first(w):
        for kind in (0, 1, 2):
            plan[w][kind].start()

    def second(w):
        plan[w][0].wait_recv()
        for kind in (5, 4, 7):
            plan[w][kind].start()
        plan[w][1].wait_recv()
        for kind in (6, 3, 8):
            plan[w][kind].start()

    def third(w):
        for kind, onward in ((3, 9), (4, 10), (5, 11), (6, 12)):
            plan[w][kind].wait_recv()
            plan[w][onward].start()

    loads = [pltpu.make_async_copy(shards[w], kept[w], kept_in.at[w]) for w in range(4)]
    stores = [
        pltpu.make_async_copy(kept[w], fulls[w].at[rows_of(w, f, 0, shards[w].shape[0])], kept_out.at[w])
        for w in range(4)
    ]
    order = (1,0,2,3)
    first(order[0])
    first(order[1])
    for w in range(4):
        loads[w].start()
    for w in range(4):
        loads[w].wait()
        stores[w].start()
    second(order[0])
    first(order[2])
    second(order[1])
    first(order[3])
    third(order[0])
    second(order[2])
    third(order[1])
    second(order[3])
    third(order[2])
    third(order[3])
    for w in range(4):
        stores[w].wait()
        for kind in range(GATHER_KINDS):
            if kind == 2 or kind >= 7:
                plan[w][kind].wait_recv()
            plan[w][kind].wait_send()


def gather_weights(weights, parts):
    return pl.pallas_call(
        gather_kernel,
        out_shape=[
            jax.ShapeDtypeStruct((w.shape[0] * parts, w.shape[1]), w.dtype) for w in weights
        ],
        in_specs=[pl.BlockSpec(memory_space=ANY)] * 4,
        out_specs=[pl.BlockSpec(memory_space=ANY)] * 4,
        scratch_shapes=[pltpu.VMEM(w.shape, w.dtype) for w in weights]
        + [
            pltpu.SemaphoreType.DMA((4,)),
            pltpu.SemaphoreType.DMA((4,)),
            pltpu.SemaphoreType.DMA((4, GATHER_KINDS)),
            pltpu.SemaphoreType.DMA((4, GATHER_KINDS)),
        ],
        compiler_params=pltpu.CompilerParams(
            collective_id=1, has_side_effects=True, vmem_limit_bytes=60 * 1024 * 1024
        ),
        name="gather_weights",
    )(*weights)


CHUNKS = 12
LEFTS = 7
RIGHTS = 9
BLOCK = 128
WIDE = 1024
LAST = 7


def left_of(t):
    return jnp.where(t < 4, t, jnp.where(t < 8, 4, jnp.where(t < 11, 5, 6)))


def right_of(t):
    return jnp.where(t < 4, 0, t - 3)


def add_rows(target, sources, rows):
    def step(i, carry):
        at = pl.ds(pl.multiple_of(i * 16, 16), 16)
        total = sources[0][at].astype(jnp.float32)
        for source in sources[1:]:
            total = total + source[at].astype(jnp.float32)
        target[at] = total.astype(target.dtype)
        return carry

    lax.fori_loop(0, rows // 16, step, 0)


def reduce_kernel(*refs):
    activated, normed_mid, normed_in, attended, grad_mlp, grad_up_in, grad_packed, grad_attn = refs[:8]
    small, sums, small_sums = refs[8:11]
    (left, right, part, from_x, from_y, last_x, last_y, from_pair, from_far) = refs[11:20]
    small_sent, small_got = refs[20:22]
    (in_own, in_send, in_recv, rin_own, rin_send, rin_recv) = refs[22:28]
    send, recv, small_send, small_recv = refs[28:32]

    z, f, core, along_x, along_y, across = places()
    pair, far = flip(z, 1), flip(z, 2)
    at_core, at_x, at_y = (z, core), (z, along_x), (z, along_y)
    at_pair, at_far = (pair, f), (far, f)
    greet((at_core, at_x, at_y, at_pair, at_far))

    rows = grad_mlp.shape[0]
    mine = pl.ds(pl.multiple_of((f % 2) * rows, rows), rows)
    half = BLOCK // 2
    quarter = BLOCK // 4
    top, bottom = pl.ds(0, half), pl.ds(half, half)

    def left_source(i):
        if i < 4:
            return activated, 4 * BLOCK, i * BLOCK
        return (normed_mid, normed_in, attended)[i - 4], BLOCK, 0

    def right_source(i):
        if i == 0:
            return grad_mlp, 0
        if i < 5:
            return grad_up_in, (i - 1) * WIDE
        if i < 8:
            return grad_packed, (i - 5) * WIDE
        return grad_attn, 0

    def spread(index):
        return (index, flip(index, 2), flip(index, 4), flip(flip(index, 2), 4))

    def left_copies(i):
        source, stride, offset = left_source(i)
        here, there = [], []
        for slot in range(4):
            target = left.at[i, mine, pl.ds(slot * BLOCK, BLOCK)]
            columns = [
                pl.ds(pl.multiple_of(spread(index)[slot] * stride + offset, BLOCK), BLOCK)
                for index in (f, core)
            ]
            here.append(
                pltpu.make_async_copy(source.at[:, columns[0]], target, in_own.at[i, slot])
            )
            there.append(
                pltpu.make_async_remote_copy(
                    src_ref=source.at[:, columns[1]],
                    dst_ref=target,
                    send_sem=in_send.at[i, slot],
                    recv_sem=in_recv.at[i, slot],
                    device_id=at_core,
                    device_id_type=MESH,
                )
            )
        return here + there

    def right_copies(i):
        source, offset = right_source(i)
        source = source.at[:, pl.ds(offset, WIDE)]
        target = right.at[i, mine]
        return [
            pltpu.make_async_copy(source, target, rin_own.at[i]),
            pltpu.make_async_remote_copy(
                src_ref=source,
                dst_ref=target,
                send_sem=rin_send.at[i],
                recv_sem=rin_recv.at[i],
                device_id=at_core,
                device_id_type=MESH,
            ),
        ]

    lefts = [left_copies(i) for i in range(LEFTS)]
    rights = [right_copies(i) for i in range(RIGHTS)]
    new_left = {0: 0, 1: 1, 2: 2, 3: 3, 4: 4, 8: 5, 11: 6}
    new_right = {0: 0, 4: 1, 5: 2, 6: 3, 7: 4, 8: 5, 9: 6, 10: 7, 11: 8}
    for t in range(CHUNKS):
        for copy in lefts[new_left[t]] if t in new_left else ():
            copy.start()
        for copy in rights[new_right[t]] if t in new_right else ():
            copy.start()

    def remote(t, kind, source, target, peer):
        return pltpu.make_async_remote_copy(
            src_ref=source,
            dst_ref=target,
            send_sem=send.at[t, kind],
            recv_sem=recv.at[t, kind],
            device_id=peer,
            device_id_type=MESH,
        )

    keep = pl.multiple_of((z % 2) * half, half)
    give = pl.multiple_of(half - keep, half)
    keep_part = pl.multiple_of(keep + (z // 2) * quarter, quarter)
    give_part = pl.multiple_of(keep + (1 - z // 2) * quarter, quarter)

    def moved(t, kind):
        source, target, peer = (
            lambda: (part.at[t, 1, top], from_x.at[t, 0], at_x),
            lambda: (part.at[t, 3, top], from_x.at[t, 1], at_x),
            lambda: (part.at[t, 2, bottom], from_y.at[t, 0], at_y),
            lambda: (part.at[t, 3, bottom], from_y.at[t, 1], at_y),
            lambda: (part.at[t, 1, bottom], last_x.at[t], at_x),
            lambda: (part.at[t, 2, top], last_y.at[t], at_y),
            lambda: (part.at[t, 0, pl.ds(give, half)], from_pair.at[t], at_pair),
            lambda: (part.at[t, 0, pl.ds(give_part, quarter)], from_far.at[t], at_far),
            lambda: (sums.at[t, pl.ds(keep_part, quarter)],) * 2 + (at_far,),
            lambda: (sums.at[t, pl.ds(keep, half)],) * 2 + (at_pair,),
        )[kind]()
        return remote(t, kind, source, target, peer)

    def stage_product(t):
        lhs = left[left_of(t)]
        for column in range(0, WIDE, 256):
            block = lax.dot_general(
                lhs,
                right[right_of(t), :, column : column + 256],
                (((0,), (0,)), ((), ())),
                preferred_element_type=jnp.float32,
            ).astype(jnp.bfloat16)
            for slot in range(4):
                part[t, slot, :, column : column + 256] = block[slot * BLOCK : (slot + 1) * BLOCK]
        for kind in (1, 3, 0, 2):
            moved(t, kind).start()

    def stage_turn(t):
        moved(t, 1).wait_recv()
        add_rows(part.at[t, 2, top], (part.at[t, 2, top], from_x.at[t, 1]), half)
        moved(t, 5).start()
        moved(t, 3).wait_recv()
        add_rows(part.at[t, 1, bottom], (part.at[t, 1, bottom], from_y.at[t, 1]), half)
        moved(t, 4).start()

    def stage_plane(t):
        moved(t, 0).wait_recv()
        moved(t, 5).wait_recv()
        add_rows(part.at[t, 0, top], (part.at[t, 0, top], from_x.at[t, 0], last_y.at[t]), half)
        moved(t, 2).wait_recv()
        moved(t, 4).wait_recv()
        add_rows(
            part.at[t, 0, bottom], (part.at[t, 0, bottom], from_y.at[t, 0], last_x.at[t]), half
        )
        moved(t, 6).start()

    def stage_pair(t):
        moved(t, 6).wait_recv()
        target = part.at[t, 0, pl.ds(keep, half)]
        add_rows(target, (target, from_pair.at[t]), half)
        moved(t, 7).start()

    def stage_far(t):
        moved(t, 7).wait_recv()
        add_rows(
            sums.at[t, pl.ds(keep_part, quarter)],
            (part.at[t, 0, pl.ds(keep_part, quarter)], from_far.at[t]),
            quarter,
        )
        moved(t, 8).start()

    def stage_back(t):
        moved(t, 8).wait_recv()
        moved(t, 8).wait_send()
        moved(t, 9).start()

    def stage_end(t):
        moved(t, 9).wait_recv()
        for kind in (0, 1, 2, 3, 4, 5, 6, 7, 9):
            moved(t, kind).wait_send()

    peers = (at_core, at_x, at_y, at_pair, at_far)

    def small_copy(j):
        return pltpu.make_async_remote_copy(
            src_ref=small_sent.at[j],
            dst_ref=small_got.at[j],
            send_sem=small_send.at[j],
            recv_sem=small_recv.at[j],
            device_id=peers[j],
            device_id_type=MESH,
        )

    small_sent[0] = small[...]
    small_copy(0).start()
    stages = (stage_turn, stage_plane, stage_pair, stage_far, stage_back, stage_end)

    def tick(t, carry):
        for when, i in new_left.items():

            @pl.when(t == when)
            def _(i=i):
                for copy in lefts[i]:
                    copy.wait()

        for when, i in new_right.items():

            @pl.when(t == when)
            def _(i=i):
                for copy in rights[i]:
                    copy.wait()

        @pl.when(t < CHUNKS)
        def _():
            stage_product(t)

        for lag, stage in enumerate(stages, 1):

            @pl.when((t >= lag) & (t < CHUNKS + lag))
            def _(lag=lag, stage=stage):
                stage(t - lag)

        for j in range(5):

            @pl.when(t == j)
            def _(j=j):
                small_copy(j).wait()
                total = small_sent[j] + small_got[j]
                if j < 4:
                    small_sent[j + 1] = total
                    small_copy(j + 1).start()
                else:
                    small_sums[...] = total

        return carry

    lax.fori_loop(0, CHUNKS + len(stages), tick, 0)


def reduce_gradients(lefts, rights, small):
    rows = lefts[0].shape[0]
    bf16, dma = jnp.bfloat16, pltpu.SemaphoreType.DMA
    return pl.pallas_call(
        reduce_kernel,
        out_shape=[
            jax.ShapeDtypeStruct((CHUNKS, BLOCK, WIDE), bf16),
            jax.ShapeDtypeStruct(small.shape, jnp.float32),
        ],
        in_specs=[pl.BlockSpec(memory_space=ANY)] * 8 + [pl.BlockSpec(memory_space=pltpu.VMEM)],
        out_specs=[pl.BlockSpec(memory_space=pltpu.VMEM)] * 2,
        scratch_shapes=[
            pltpu.VMEM((LEFTS, 2 * rows, 4 * BLOCK), bf16),
            pltpu.VMEM((RIGHTS, 2 * rows, WIDE), bf16),
            pltpu.VMEM((CHUNKS, 4, BLOCK, WIDE), bf16),
            pltpu.VMEM((CHUNKS, 2, BLOCK // 2, WIDE), bf16),
            pltpu.VMEM((CHUNKS, 2, BLOCK // 2, WIDE), bf16),
            pltpu.VMEM((CHUNKS, BLOCK // 2, WIDE), bf16),
            pltpu.VMEM((CHUNKS, BLOCK // 2, WIDE), bf16),
            pltpu.VMEM((CHUNKS, BLOCK // 2, WIDE), bf16),
            pltpu.VMEM((CHUNKS, BLOCK // 4, WIDE), bf16),
            pltpu.VMEM((5,) + small.shape, jnp.float32),
            pltpu.VMEM((5,) + small.shape, jnp.float32),
            dma((LEFTS, 4)),
            dma((LEFTS, 4)),
            dma((LEFTS, 4)),
            dma((RIGHTS,)),
            dma((RIGHTS,)),
            dma((RIGHTS,)),
            dma((CHUNKS, 10)),
            dma((CHUNKS, 10)),
            dma((5,)),
            dma((5,)),
        ],
        compiler_params=pltpu.CompilerParams(
            collective_id=2, has_side_effects=True, vmem_limit_bytes=60 * 1024 * 1024
        ),
        name="reduce_gradients",
    )(*lefts, *rights, small)


def put_rows(tokens, rows, positions):
    hit = lax.broadcasted_iota(jnp.int32, (tokens.shape[0], positions.shape[0]), 0) == positions[None]
    moved = jnp.dot(hit.astype(jnp.bfloat16), rows, preferred_element_type=jnp.float32)
    return jnp.where(jnp.any(hit, axis=1, keepdims=True), moved.astype(jnp.bfloat16), tokens)


def per_device(
    hidden, cotangent, route_pos, route_doc, w_qkv, w_out, w_up, w_down, router, gain_one, gain_two
):
    positions = route_pos[0]
    documents = route_doc[0]
    live_mask = (documents < 2).astype(jnp.float32)[:, None]
    weights = gather_weights((w_qkv, w_out, w_up, w_down), 8)
    state = forward(hidden, positions, documents, weights, router, gain_one, gain_two)
    full_qkv, full_out, full_up, full_down = weights
    (
        routed,
        router_out,
        normed_in,
        heads,
        prob_rows,
        prob_low,
        attended,
        attn_out,
        middle,
        normed_mid,
        up_in,
        activated,
        mlp_out,
    ) = state
    row_count = routed.shape[0]
    branch_out = attn_out + mlp_out
    added = live_mask * router_out[:, None] * branch_out
    output = put_rows(hidden, (routed + added).astype(jnp.bfloat16), positions)
    taken = cotangent[positions].astype(jnp.float32)
    grad_add = live_mask * taken
    grad_branch = grad_add * router_out[:, None]
    grad_score = jnp.sum(grad_add * branch_out, axis=-1)
    grad_mlp = grad_branch.astype(jnp.bfloat16)
    grad_act = jnp.dot(grad_mlp, full_down.T, preferred_element_type=jnp.float32)
    _, gelu_pull = jax.vjp(jax.nn.gelu, up_in)
    grad_up_in = gelu_pull(grad_act)[0].astype(jnp.bfloat16)
    grad_norm_mid = jnp.dot(grad_up_in, full_up.T, preferred_element_type=jnp.float32)
    _, second_pull = jax.vjp(rms_scale, middle, gain_two)
    grad_middle, grad_gain_two = second_pull(grad_norm_mid)
    grad_attn = (grad_branch + grad_middle).astype(jnp.bfloat16)
    grad_attended = jnp.dot(grad_attn, full_out.T, preferred_element_type=jnp.float32).astype(
        jnp.bfloat16
    )
    grad_attended = grad_attended.reshape(row_count, HEADS, HEAD)
    grad_prob = jnp.einsum(
        "qhd,khd->hqk", grad_attended, heads[:, 2], preferred_element_type=jnp.float32
    )
    grad_value = jnp.einsum(
        "hqk,qhd->khd", prob_low, grad_attended, preferred_element_type=jnp.float32
    )
    row_dot = jnp.sum(grad_prob * prob_rows, axis=-1, keepdims=True)
    grad_scores = (prob_rows * (grad_prob - row_dot)).astype(jnp.bfloat16)
    grad_query = (
        jnp.einsum("hqk,khd->qhd", grad_scores, heads[:, 1], preferred_element_type=jnp.float32)
        * 0.125
    )
    grad_key = (
        jnp.einsum("hqk,qhd->khd", grad_scores, heads[:, 0], preferred_element_type=jnp.float32)
        * 0.125
    )
    grad_packed = jnp.stack([grad_query, grad_key, grad_value], axis=1).reshape(row_count, 3 * D)
    grad_packed = grad_packed.astype(jnp.bfloat16)
    grad_norm_in = jnp.dot(grad_packed, full_qkv.T, preferred_element_type=jnp.float32)
    _, first_pull = jax.vjp(rms_scale, routed, gain_one)
    grad_routed, grad_gain_one = first_pull(grad_norm_in)
    grad_routed = grad_routed + grad_middle + grad_score[:, None] * router[None, :]
    grad_router = jnp.dot(grad_score, routed, precision=lax.Precision.HIGHEST)
    grad_hidden = put_rows(cotangent, (taken + grad_routed).astype(jnp.bfloat16), positions)
    small = jnp.stack([grad_router, grad_gain_one, grad_gain_two] + [jnp.zeros_like(grad_router)] * 5)
    sums, small_sums = reduce_gradients(
        (activated, normed_mid, normed_in, attended),
        (grad_mlp, grad_up_in, grad_packed, grad_attn),
        small,
    )
    wide = sums.astype(jnp.float32)
    return (
        output,
        grad_hidden,
        wide[8:11].transpose(1, 0, 2).reshape(w_qkv.shape),
        wide[11],
        wide[4:8].transpose(1, 0, 2).reshape(w_up.shape),
        wide[:4].reshape(w_down.shape),
        small_sums[0],
        small_sums[1],
        small_sums[2],
    )


def solution(mesh):
    paired = dict(mesh.shape) == {"dp": 4, "fsdp": 8}
    tokens, weights = P(("dp", "fsdp"), None), P("fsdp", None)
    return jax.shard_map(
        per_device if paired else general_device,
        mesh=mesh,
        in_specs=(tokens,) * 4 + (weights,) * 4 + (P(),) * 3,
        out_specs=(tokens,) * 2 + (weights,) * 4 + (P(),) * 3,
        check_vma=False,
    )
```

```python
import functools

import jax
import jax.numpy as jnp
from jax import lax
from jax.experimental import pallas as pl
from jax.experimental.pallas import tpu as pltpu
from jax.sharding import PartitionSpec as P

D = 1024
HEADS = 16
HEAD = 64


EPS = 1e-06


def rms_scale(values, gain_vec):
    return values * lax.rsqrt(jnp.mean(values * values, axis=-1, keepdims=True) + EPS) * gain_vec


def forward(tokens, positions, documents, weights, router, gain_one, gain_two):
    full_qkv, full_out, full_up, full_down = weights
    routed = tokens[positions].astype(jnp.float32)
    row_count = routed.shape[0]
    router_out = jnp.dot(routed, router, precision=lax.Precision.HIGHEST)
    normed_in = rms_scale(routed, gain_one).astype(jnp.bfloat16)
    packed = jnp.dot(normed_in, full_qkv, preferred_element_type=jnp.float32).astype(jnp.bfloat16)
    heads = packed.reshape(row_count, 3, HEADS, HEAD)
    allowed = (documents[:, None] == documents[None, :]) & (
        positions[None, :] <= positions[:, None]
    )
    scores = (
        jnp.einsum("qhd,khd->hqk", heads[:, 0], heads[:, 1], preferred_element_type=jnp.float32)
        * 0.125
    )
    scores = jnp.where(allowed[None], scores, -1000000000.0)
    row_max = jnp.max(scores, axis=-1, keepdims=True)
    log_total = row_max + jnp.log(jnp.sum(jnp.exp(scores - row_max), axis=-1, keepdims=True))
    prob_rows = jnp.exp(scores - log_total)
    prob_low = prob_rows.astype(jnp.bfloat16)
    attended = jnp.einsum("hqk,khd->qhd", prob_low, heads[:, 2], preferred_element_type=jnp.float32)
    attended = attended.reshape(row_count, D).astype(jnp.bfloat16)
    attn_out = jnp.dot(attended, full_out, preferred_element_type=jnp.float32)
    middle = routed + attn_out
    normed_mid = rms_scale(middle, gain_two).astype(jnp.bfloat16)
    up_in = jnp.dot(normed_mid, full_up, preferred_element_type=jnp.float32)
    activated = jax.nn.gelu(up_in).astype(jnp.bfloat16)
    mlp_out = jnp.dot(activated, full_down, preferred_element_type=jnp.float32)
    return (
        routed,
        router_out,
        normed_in,
        heads,
        prob_rows,
        prob_low,
        attended,
        attn_out,
        middle,
        normed_mid,
        up_in,
        activated,
        mlp_out,
    )


def general_device(
    hidden, cotangent, route_pos, route_doc, w_qkv, w_out, w_up, w_down, router, gain_one, gain_two
):
    positions = route_pos[0]
    documents = route_doc[0]
    live_mask = (documents < 2).astype(jnp.float32)[:, None]
    gathered = (
        lax.all_gather(w_qkv, "fsdp", axis=0, tiled=True),
        lax.all_gather(w_out, "fsdp", axis=0, tiled=True),
        lax.all_gather(w_up, "fsdp", axis=0, tiled=True),
        lax.all_gather(w_down, "fsdp", axis=0, tiled=True),
    )
    state = forward(hidden, positions, documents, gathered, router, gain_one, gain_two)
    attn_first = state[7]
    mlp_first = state[12]
    added = live_mask * state[1][:, None] * (attn_first + mlp_first)
    output = hidden.astype(jnp.float32).at[positions].add(added).astype(jnp.bfloat16)
    weights = (
        lax.all_gather(w_qkv, "fsdp", axis=0, tiled=True),
        lax.all_gather(w_out, "fsdp", axis=0, tiled=True),
        lax.all_gather(w_up, "fsdp", axis=0, tiled=True),
        lax.all_gather(w_down, "fsdp", axis=0, tiled=True),
    )
    state = forward(hidden, positions, documents, weights, router, gain_one, gain_two)
    full_qkv, full_out, full_up, full_down = weights
    (
        routed,
        router_out,
        normed_in,
        heads,
        prob_rows,
        prob_low,
        attended,
        attn_out,
        middle,
        normed_mid,
        up_in,
        activated,
        mlp_out,
    ) = state
    row_count = routed.shape[0]
    branch_out = attn_out + mlp_out
    grad_add = live_mask * cotangent[positions].astype(jnp.float32)
    grad_branch = grad_add * router_out[:, None]
    grad_score = jnp.sum(grad_add * branch_out, axis=-1)
    grad_mlp = grad_branch.astype(jnp.bfloat16)
    grad_down = jnp.dot(activated.T, grad_mlp, preferred_element_type=jnp.float32)
    grad_act = jnp.dot(grad_mlp, full_down.T, preferred_element_type=jnp.float32)
    _, gelu_pull = jax.vjp(jax.nn.gelu, up_in)
    grad_up_in = gelu_pull(grad_act)[0].astype(jnp.bfloat16)
    grad_up = jnp.dot(normed_mid.T, grad_up_in, preferred_element_type=jnp.float32)
    grad_norm_mid = jnp.dot(grad_up_in, full_up.T, preferred_element_type=jnp.float32)
    _, second_pull = jax.vjp(rms_scale, middle, gain_two)
    grad_middle, grad_gain_two = second_pull(grad_norm_mid)
    grad_attn = (grad_branch + grad_middle).astype(jnp.bfloat16)
    grad_out = jnp.dot(attended.T, grad_attn, preferred_element_type=jnp.float32)
    grad_attended = jnp.dot(grad_attn, full_out.T, preferred_element_type=jnp.float32).astype(
        jnp.bfloat16
    )
    grad_attended = grad_attended.reshape(row_count, HEADS, HEAD)
    grad_prob = jnp.einsum(
        "qhd,khd->hqk", grad_attended, heads[:, 2], preferred_element_type=jnp.float32
    )
    grad_value = jnp.einsum(
        "hqk,qhd->khd", prob_low, grad_attended, preferred_element_type=jnp.float32
    )
    row_dot = jnp.sum(grad_prob * prob_rows, axis=-1, keepdims=True)
    grad_scores = (prob_rows * (grad_prob - row_dot)).astype(jnp.bfloat16)
    grad_query = (
        jnp.einsum("hqk,khd->qhd", grad_scores, heads[:, 1], preferred_element_type=jnp.float32)
        * 0.125
    )
    grad_key = (
        jnp.einsum("hqk,qhd->khd", grad_scores, heads[:, 0], preferred_element_type=jnp.float32)
        * 0.125
    )
    grad_packed = jnp.stack([grad_query, grad_key, grad_value], axis=1).reshape(row_count, 3 * D)
    grad_packed = grad_packed.astype(jnp.bfloat16)
    grad_qkv = jnp.dot(normed_in.T, grad_packed, preferred_element_type=jnp.float32)
    grad_norm_in = jnp.dot(grad_packed, full_qkv.T, preferred_element_type=jnp.float32)
    _, first_pull = jax.vjp(rms_scale, routed, gain_one)
    grad_routed, grad_gain_one = first_pull(grad_norm_in)
    grad_routed = grad_routed + grad_middle + grad_score[:, None] * router[None, :]
    grad_router = jnp.dot(grad_score, routed, precision=lax.Precision.HIGHEST)
    grad_hidden = cotangent.astype(jnp.float32).at[positions].add(grad_routed).astype(jnp.bfloat16)
    shard_sums = (
        lax.psum_scatter(grad_qkv.astype(jnp.bfloat16), "fsdp", scatter_dimension=0, tiled=True),
        lax.psum_scatter(grad_out.astype(jnp.bfloat16), "fsdp", scatter_dimension=0, tiled=True),
        lax.psum_scatter(grad_up.astype(jnp.bfloat16), "fsdp", scatter_dimension=0, tiled=True),
        lax.psum_scatter(grad_down.astype(jnp.bfloat16), "fsdp", scatter_dimension=0, tiled=True),
    )
    final_sums = lax.psum((shard_sums[0], shard_sums[1], shard_sums[2], shard_sums[3]), "dp")
    small_sums = lax.psum((grad_router, grad_gain_one, grad_gain_two), ("dp", "fsdp"))
    return (
        output,
        grad_hidden,
        final_sums[0].astype(jnp.float32),
        final_sums[1].astype(jnp.float32),
        final_sums[2].astype(jnp.float32),
        final_sums[3].astype(jnp.float32),
        small_sums[0],
        small_sums[1],
        small_sums[2],
    )


MESH = pl.DeviceIdType.MESH
ANY = pl.ANY


def flip(index, stride):
    return index + stride - 2 * stride * ((index // stride) % 2)


def places():
    z = lax.axis_index("dp")
    f = lax.axis_index("fsdp")
    return z, f, flip(f, 1), flip(f, 2), flip(f, 4), flip(flip(f, 2), 4)


def greet(peers):
    barrier = pltpu.get_barrier_semaphore()
    for peer in peers:
        pl.semaphore_signal(barrier, inc=1, device_id=peer, device_id_type=MESH)
    pl.semaphore_wait(barrier, len(peers))


GATHER_KINDS = 13


def gather_kernel(*refs):
    shards, fulls, kept = refs[0:4], refs[4:8], refs[8:12]
    kept_in, kept_out, send, recv = refs[12:16]
    z, f, core, along_x, along_y, across = places()
    pair = flip(z, 1)
    at_core, at_x, at_y, at_z = (z, core), (z, along_x), (z, along_y), (pair, f)
    greet((at_core, at_x, at_y, at_z))

    def rows_of(w, origin, start, size):
        rows = shards[w].shape[0]
        return pl.ds(pl.multiple_of(origin * rows + start, 16), size)

    def copy(w, kind, source, origin, start, size, peer):
        return pltpu.make_async_remote_copy(
            src_ref=source,
            dst_ref=fulls[w].at[rows_of(w, origin, start, size)],
            send_sem=send.at[w, kind],
            recv_sem=recv.at[w, kind],
            device_id=peer,
            device_id_type=MESH,
        )

    def own(w, kind, start, size, peer):
        source = shards[w].at[pl.ds(pl.multiple_of(start, 16), size)]
        return copy(w, kind, source, f, start, size, peer)

    def passed(w, kind, origin, start, size, peer):
        return copy(w, kind, fulls[w].at[rows_of(w, origin, start, size)], origin, start, size, peer)

    plan = []
    for w in range(4):
        rows = shards[w].shape[0]
        half = rows // 2
        even, odd = (z % 2) * half, (1 - z % 2) * half
        plan.append(
            [
                own(w, 0, even, half, at_x),
                own(w, 1, odd, half, at_y),
                own(w, 2, 0, rows, at_core),
                passed(w, 3, along_y, odd, half, at_x),
                passed(w, 4, along_x, even, half, at_y),
                passed(w, 5, along_x, even, half, at_z),
                passed(w, 6, along_y, odd, half, at_z),
                passed(w, 7, along_x, even, half, at_core),
                passed(w, 8, along_y, odd, half, at_core),
                passed(w, 9, across, odd, half, at_core),
                passed(w, 10, across, even, half, at_core),
                passed(w, 11, along_x, odd, half, at_core),
                passed(w, 12, along_y, even, half, at_core),
            ]
        )

    def first(w):
        for kind in (0, 1, 2):
            plan[w][kind].start()

    def second(w):
        plan[w][0].wait_recv()
        for kind in (5, 4, 7):
            plan[w][kind].start()
        plan[w][1].wait_recv()
        for kind in (6, 3, 8):
            plan[w][kind].start()

    def third(w):
        for kind, onward in ((3, 9), (4, 10), (5, 11), (6, 12)):
            plan[w][kind].wait_recv()
            plan[w][onward].start()

    loads = [pltpu.make_async_copy(shards[w], kept[w], kept_in.at[w]) for w in range(4)]
    stores = [
        pltpu.make_async_copy(kept[w], fulls[w].at[rows_of(w, f, 0, shards[w].shape[0])], kept_out.at[w])
        for w in range(4)
    ]
    order = (1,0,2,3)
    first(order[0])
    first(order[1])
    for w in range(4):
        loads[w].start()
    for w in range(4):
        loads[w].wait()
        stores[w].start()
    second(order[0])
    first(order[2])
    second(order[1])
    first(order[3])
    third(order[0])
    second(order[2])
    third(order[1])
    second(order[3])
    third(order[2])
    third(order[3])
    for w in range(4):
        stores[w].wait()
        for kind in range(GATHER_KINDS):
            if kind == 2 or kind >= 7:
                plan[w][kind].wait_recv()
            plan[w][kind].wait_send()


def gather_weights(weights, parts):
    return pl.pallas_call(
        gather_kernel,
        out_shape=[
            jax.ShapeDtypeStruct((w.shape[0] * parts, w.shape[1]), w.dtype) for w in weights
        ],
        in_specs=[pl.BlockSpec(memory_space=ANY)] * 4,
        out_specs=[pl.BlockSpec(memory_space=ANY)] * 4,
        scratch_shapes=[pltpu.VMEM(w.shape, w.dtype) for w in weights]
        + [
            pltpu.SemaphoreType.DMA((4,)),
            pltpu.SemaphoreType.DMA((4,)),
            pltpu.SemaphoreType.DMA((4, GATHER_KINDS)),
            pltpu.SemaphoreType.DMA((4, GATHER_KINDS)),
        ],
        compiler_params=pltpu.CompilerParams(
            collective_id=1, has_side_effects=True, vmem_limit_bytes=60 * 1024 * 1024
        ),
        name="gather_weights",
    )(*weights)


CHUNKS = 24
LAGS = (1, 2, 3, 4, 5, 6)
LEFTS = 7
RIGHTS = 9
BLOCK = 128
WIDE = 512
FULL = 1024
LAST = 7


def left_of(t):
    return jnp.where(t < 8, t // 2, jnp.where(t < 16, 4, jnp.where(t < 22, 5, 6)))


def right_of(t):
    return jnp.where(t < 8, 0, t // 2 - 3)


def add_rows(target, sources, rows):
    def step(i, carry):
        at = pl.ds(pl.multiple_of(i * 16, 16), 16)
        total = sources[0][at].astype(jnp.float32)
        for source in sources[1:]:
            total = total + source[at].astype(jnp.float32)
        target[at] = total.astype(target.dtype)
        return carry

    lax.fori_loop(0, rows // 16, step, 0)


def reduce_kernel(*refs):
    activated, normed_mid, normed_in, attended, grad_mlp, grad_up_in, grad_packed, grad_attn = refs[:8]
    small, out_down, out_up, out_qkv, out_out, small_sums = refs[8:14]
    sums, stored = refs[35:37]
    (left, right, part, from_x, from_y, last_x, last_y, from_pair, from_far) = refs[14:23]
    small_sent, small_got = refs[23:25]
    (in_own, in_send, in_recv, rin_own, rin_send, rin_recv) = refs[25:31]
    send, recv, small_send, small_recv = refs[31:35]

    z, f, core, along_x, along_y, across = places()
    pair, far = flip(z, 1), 3 - z
    inner = (z == 1) | (z == 2)
    outer = (z == 0) | (z == 3)
    at_core, at_x, at_y = (z, core), (z, along_x), (z, along_y)
    at_pair, at_far = (pair, f), (far, f)
    greet((at_core, at_x, at_y, at_pair, at_far))

    rows = grad_mlp.shape[0]
    mine = pl.ds(pl.multiple_of((f % 2) * rows, rows), rows)
    half = BLOCK // 2
    top, bottom = pl.ds(0, half), pl.ds(half, half)

    def left_source(i):
        if i < 4:
            return activated, 4 * BLOCK, i * BLOCK
        return (normed_mid, normed_in, attended)[i - 4], BLOCK, 0

    def right_source(i):
        if i == 0:
            return grad_mlp, 0
        if i < 5:
            return grad_up_in, (i - 1) * FULL
        if i < 8:
            return grad_packed, (i - 5) * FULL
        return grad_attn, 0

    def spread(index):
        return (index, flip(index, 2), flip(index, 4), flip(flip(index, 2), 4))

    def left_copies(i):
        source, stride, offset = left_source(i)
        here, there = [], []
        for slot in range(4):
            target = left.at[i, mine, pl.ds(slot * BLOCK, BLOCK)]
            columns = [
                pl.ds(pl.multiple_of(spread(index)[slot] * stride + offset, BLOCK), BLOCK)
                for index in (f, core)
            ]
            here.append(
                pltpu.make_async_copy(source.at[:, columns[0]], target, in_own.at[i, slot])
            )
            there.append(
                pltpu.make_async_remote_copy(
                    src_ref=source.at[:, columns[1]],
                    dst_ref=target,
                    send_sem=in_send.at[i, slot],
                    recv_sem=in_recv.at[i, slot],
                    device_id=at_core,
                    device_id_type=MESH,
                )
            )
        return here + there

    def right_copies(i):
        source, offset = right_source(i)
        source = source.at[:, pl.ds(offset, FULL)]
        target = right.at[i, mine]
        return [
            pltpu.make_async_copy(source, target, rin_own.at[i]),
            pltpu.make_async_remote_copy(
                src_ref=source,
                dst_ref=target,
                send_sem=rin_send.at[i],
                recv_sem=rin_recv.at[i],
                device_id=at_core,
                device_id_type=MESH,
            ),
        ]

    lefts = [left_copies(i) for i in range(LEFTS)]
    rights = [right_copies(i) for i in range(RIGHTS)]
    new_left = {0: 0, 2: 1, 4: 2, 6: 3, 8: 4, 16: 5, 22: 6}
    new_right = {0: 0, 8: 1, 10: 2, 12: 3, 14: 4, 16: 5, 18: 6, 20: 7, 22: 8}
    for t in range(CHUNKS):
        for copy in lefts[new_left[t]] if t in new_left else ():
            copy.start()
        for copy in rights[new_right[t]] if t in new_right else ():
            copy.start()

    def remote(t, kind, source, target, peer):
        return pltpu.make_async_remote_copy(
            src_ref=source,
            dst_ref=target,
            send_sem=send.at[t, kind],
            recv_sem=recv.at[t, kind],
            device_id=peer,
            device_id_type=MESH,
        )

    def moved(t, kind):
        source, target, peer = (
            lambda: (part.at[t, 1, top], from_x.at[t, 0], at_x),
            lambda: (part.at[t, 3, top], from_x.at[t, 1], at_x),
            lambda: (part.at[t, 2, bottom], from_y.at[t, 0], at_y),
            lambda: (part.at[t, 3, bottom], from_y.at[t, 1], at_y),
            lambda: (part.at[t, 1, bottom], last_x.at[t], at_x),
            lambda: (part.at[t, 2, top], last_y.at[t], at_y),
            lambda: (part.at[t, 0], from_pair.at[t], at_pair),
            lambda: (part.at[t, 0], from_far.at[t], at_far),
            lambda: (sums.at[t], sums.at[t], at_pair),
        )[kind]()
        return remote(t, kind, source, target, peer)

    def stage_product(t):
        lhs = left[left_of(t)]
        for column in range(0, WIDE, 256):
            block = lax.dot_general(
                lhs,
                right[right_of(t), :, pl.ds(pl.multiple_of((t % 2) * WIDE + column, 256), 256)],
                (((0,), (0,)), ((), ())),
                preferred_element_type=jnp.float32,
            ).astype(jnp.bfloat16)
            for slot in range(4):
                part[t, slot, :, column : column + 256] = block[slot * BLOCK : (slot + 1) * BLOCK]
        for kind in (1, 3, 0, 2):
            moved(t, kind).start()

    def stage_turn(t):
        moved(t, 1).wait_recv()
        add_rows(part.at[t, 2, top], (part.at[t, 2, top], from_x.at[t, 1]), half)
        moved(t, 5).start()
        moved(t, 3).wait_recv()
        add_rows(part.at[t, 1, bottom], (part.at[t, 1, bottom], from_y.at[t, 1]), half)
        moved(t, 4).start()

    def stage_plane(t):
        moved(t, 0).wait_recv()
        moved(t, 5).wait_recv()
        add_rows(part.at[t, 0, top], (part.at[t, 0, top], from_x.at[t, 0], last_y.at[t]), half)
        moved(t, 2).wait_recv()
        moved(t, 4).wait_recv()
        add_rows(
            part.at[t, 0, bottom], (part.at[t, 0, bottom], from_y.at[t, 0], last_x.at[t]), half
        )

        @pl.when(outer)
        def _():
            moved(t, 6).start()

    def stage_pair(t):
        @pl.when(inner)
        def _():
            moved(t, 6).wait_recv()
            add_rows(part.at[t, 0], (part.at[t, 0], from_pair.at[t]), BLOCK)
            moved(t, 7).start()

    def stage_far(t):
        @pl.when(inner)
        def _():
            moved(t, 7).wait_recv()
            add_rows(sums.at[t], (part.at[t, 0], from_far.at[t]), BLOCK)
            moved(t, 8).start()

    def stage_end(t):
        @pl.when(inner)
        def _():
            moved(t, 7).wait_send()
            moved(t, 8).wait_send()

        @pl.when(outer)
        def _():
            moved(t, 6).wait_send()
            moved(t, 8).wait_recv()

        for kind in range(6):
            moved(t, kind).wait_send()

        store(t, True)

    def store(t, begin):
        for low, high, target in (
            (0, 8, lambda i: out_down.at[pl.ds(pl.multiple_of(i // 2 * BLOCK, BLOCK), BLOCK), columns(i % 2)]),
            (8, 16, lambda i: out_up.at[:, columns(i)]),
            (16, 22, lambda i: out_qkv.at[:, columns(i)]),
            (22, 24, lambda i: out_out.at[:, columns(i)]),
        ):

            @pl.when((t >= low) & (t < high))
            def _(low=low, target=target):
                copy = pltpu.make_async_copy(sums.at[t], target(t - low), stored.at[t])
                copy.start() if begin else copy.wait()

    def columns(i):
        return pl.ds(pl.multiple_of(i * WIDE, WIDE), WIDE)

    def stage_stored(t):
        store(t, False)

    peers = (at_core, at_x, at_y, at_pair, at_far)

    def small_copy(j):
        return pltpu.make_async_remote_copy(
            src_ref=small_sent.at[j],
            dst_ref=small_got.at[j],
            send_sem=small_send.at[j],
            recv_sem=small_recv.at[j],
            device_id=peers[j],
            device_id_type=MESH,
        )

    small_sent[0] = small[...]
    small_copy(0).start()
    stages = (stage_turn, stage_plane, stage_pair, stage_far, stage_end, stage_stored)

    def tick(t, carry):
        for when, i in new_left.items():

            @pl.when(t == when)
            def _(i=i):
                for copy in lefts[i]:
                    copy.wait()

        for when, i in new_right.items():

            @pl.when(t == when)
            def _(i=i):
                for copy in rights[i]:
                    copy.wait()

        @pl.when(t < CHUNKS)
        def _():
            stage_product(t)

        for lag, stage in zip(LAGS, stages):

            @pl.when((t >= lag) & (t < CHUNKS + lag))
            def _(lag=lag, stage=stage):
                stage(t - lag)

        for j in range(5):

            @pl.when(t == j)
            def _(j=j):
                small_copy(j).wait()
                total = small_sent[j] + small_got[j]
                if j < 4:
                    small_sent[j + 1] = total
                    small_copy(j + 1).start()
                else:
                    small_sums[...] = total

        return carry

    lax.fori_loop(0, CHUNKS + LAGS[-1], tick, 0)


def reduce_gradients(lefts, rights, small):
    rows = lefts[0].shape[0]
    bf16, dma = jnp.bfloat16, pltpu.SemaphoreType.DMA
    return pl.pallas_call(
        reduce_kernel,
        out_shape=[
            jax.ShapeDtypeStruct((4 * BLOCK, FULL), bf16),
            jax.ShapeDtypeStruct((BLOCK, 4 * FULL), bf16),
            jax.ShapeDtypeStruct((BLOCK, 3 * FULL), bf16),
            jax.ShapeDtypeStruct((BLOCK, FULL), bf16),
            jax.ShapeDtypeStruct(small.shape, jnp.float32),
        ],
        in_specs=[pl.BlockSpec(memory_space=ANY)] * 8 + [pl.BlockSpec(memory_space=pltpu.VMEM)],
        out_specs=[pl.BlockSpec(memory_space=ANY)] * 4 + [pl.BlockSpec(memory_space=pltpu.VMEM)],
        scratch_shapes=[
            pltpu.VMEM((LEFTS, 2 * rows, 4 * BLOCK), bf16),
            pltpu.VMEM((RIGHTS, 2 * rows, FULL), bf16),
            pltpu.VMEM((CHUNKS, 4, BLOCK, WIDE), bf16),
            pltpu.VMEM((CHUNKS, 2, BLOCK // 2, WIDE), bf16),
            pltpu.VMEM((CHUNKS, 2, BLOCK // 2, WIDE), bf16),
            pltpu.VMEM((CHUNKS, BLOCK // 2, WIDE), bf16),
            pltpu.VMEM((CHUNKS, BLOCK // 2, WIDE), bf16),
            pltpu.VMEM((CHUNKS, BLOCK, WIDE), bf16),
            pltpu.VMEM((CHUNKS, BLOCK, WIDE), bf16),
            pltpu.VMEM((5,) + small.shape, jnp.float32),
            pltpu.VMEM((5,) + small.shape, jnp.float32),
            dma((LEFTS, 4)),
            dma((LEFTS, 4)),
            dma((LEFTS, 4)),
            dma((RIGHTS,)),
            dma((RIGHTS,)),
            dma((RIGHTS,)),
            dma((CHUNKS, 9)),
            dma((CHUNKS, 9)),
            dma((5,)),
            dma((5,)),
            pltpu.VMEM((CHUNKS, BLOCK, WIDE), bf16),
            dma((CHUNKS,)),
        ],
        compiler_params=pltpu.CompilerParams(
            collective_id=2, has_side_effects=True, vmem_limit_bytes=60 * 1024 * 1024
        ),
        name="reduce_gradients",
    )(*lefts, *rights, small)


def put_rows(tokens, rows, positions):
    hit = lax.broadcasted_iota(jnp.int32, (tokens.shape[0], positions.shape[0]), 0) == positions[None]
    moved = jnp.dot(hit.astype(jnp.bfloat16), rows, preferred_element_type=jnp.float32)
    return jnp.where(jnp.any(hit, axis=1, keepdims=True), moved.astype(jnp.bfloat16), tokens)


def per_device(
    hidden, cotangent, route_pos, route_doc, w_qkv, w_out, w_up, w_down, router, gain_one, gain_two
):
    positions = route_pos[0]
    documents = route_doc[0]
    live_mask = (documents < 2).astype(jnp.float32)[:, None]
    weights = gather_weights((w_qkv, w_out, w_up, w_down), 8)
    state = forward(hidden, positions, documents, weights, router, gain_one, gain_two)
    full_qkv, full_out, full_up, full_down = weights
    (
        routed,
        router_out,
        normed_in,
        heads,
        prob_rows,
        prob_low,
        attended,
        attn_out,
        middle,
        normed_mid,
        up_in,
        activated,
        mlp_out,
    ) = state
    row_count = routed.shape[0]
    branch_out = attn_out + mlp_out
    added = live_mask * router_out[:, None] * branch_out
    output = put_rows(hidden, (routed + added).astype(jnp.bfloat16), positions)
    taken = cotangent[positions].astype(jnp.float32)
    grad_add = live_mask * taken
    grad_branch = grad_add * router_out[:, None]
    grad_score = jnp.sum(grad_add * branch_out, axis=-1)
    grad_mlp = grad_branch.astype(jnp.bfloat16)
    grad_act = jnp.dot(grad_mlp, full_down.T, preferred_element_type=jnp.float32)
    _, gelu_pull = jax.vjp(jax.nn.gelu, up_in)
    grad_up_in = gelu_pull(grad_act)[0].astype(jnp.bfloat16)
    grad_norm_mid = jnp.dot(grad_up_in, full_up.T, preferred_element_type=jnp.float32)
    _, second_pull = jax.vjp(rms_scale, middle, gain_two)
    grad_middle, grad_gain_two = second_pull(grad_norm_mid)
    grad_attn = (grad_branch + grad_middle).astype(jnp.bfloat16)
    grad_attended = jnp.dot(grad_attn, full_out.T, preferred_element_type=jnp.float32).astype(
        jnp.bfloat16
    )
    grad_attended = grad_attended.reshape(row_count, HEADS, HEAD)
    grad_prob = jnp.einsum(
        "qhd,khd->hqk", grad_attended, heads[:, 2], preferred_element_type=jnp.float32
    )
    grad_value = jnp.einsum(
        "hqk,qhd->khd", prob_low, grad_attended, preferred_element_type=jnp.float32
    )
    row_dot = jnp.sum(grad_prob * prob_rows, axis=-1, keepdims=True)
    grad_scores = (prob_rows * (grad_prob - row_dot)).astype(jnp.bfloat16)
    grad_query = (
        jnp.einsum("hqk,khd->qhd", grad_scores, heads[:, 1], preferred_element_type=jnp.float32)
        * 0.125
    )
    grad_key = (
        jnp.einsum("hqk,qhd->khd", grad_scores, heads[:, 0], preferred_element_type=jnp.float32)
        * 0.125
    )
    grad_packed = jnp.stack([grad_query, grad_key, grad_value], axis=1).reshape(row_count, 3 * D)
    grad_packed = grad_packed.astype(jnp.bfloat16)
    grad_norm_in = jnp.dot(grad_packed, full_qkv.T, preferred_element_type=jnp.float32)
    _, first_pull = jax.vjp(rms_scale, routed, gain_one)
    grad_routed, grad_gain_one = first_pull(grad_norm_in)
    grad_routed = grad_routed + grad_middle + grad_score[:, None] * router[None, :]
    grad_router = jnp.dot(grad_score, routed, precision=lax.Precision.HIGHEST)
    grad_hidden = put_rows(cotangent, (taken + grad_routed).astype(jnp.bfloat16), positions)
    small = jnp.stack([grad_router, grad_gain_one, grad_gain_two] + [jnp.zeros_like(grad_router)] * 5)
    *sums, small_sums = reduce_gradients(
        (activated, normed_mid, normed_in, attended),
        (grad_mlp, grad_up_in, grad_packed, grad_attn),
        small,
    )
    sum_down, sum_up, sum_qkv, sum_out = (total.astype(jnp.float32) for total in sums)
    return (
        output,
        grad_hidden,
        sum_qkv,
        sum_out,
        sum_up,
        sum_down,
        small_sums[0],
        small_sums[1],
        small_sums[2],
    )


def solution(mesh):
    paired = dict(mesh.shape) == {"dp": 4, "fsdp": 8}
    tokens, weights = P(("dp", "fsdp"), None), P("fsdp", None)
    return jax.shard_map(
        per_device if paired else general_device,
        mesh=mesh,
        in_specs=(tokens,) * 4 + (weights,) * 4 + (P(),) * 3,
        out_specs=(tokens,) * 2 + (weights,) * 4 + (P(),) * 3,
        check_vma=False,
    )
```

```python
import functools

import jax
import jax.numpy as jnp
from jax import lax
from jax.experimental import pallas as pl
from jax.experimental.pallas import tpu as pltpu
from jax.sharding import PartitionSpec as P

D = 1024
HEADS = 16
HEAD = 64


EPS = 1e-06


def rms_scale(values, gain_vec):
    return values * lax.rsqrt(jnp.mean(values * values, axis=-1, keepdims=True) + EPS) * gain_vec


def forward(tokens, positions, documents, weights, router, gain_one, gain_two):
    full_qkv, full_out, full_up, full_down = weights
    routed = tokens[positions].astype(jnp.float32)
    row_count = routed.shape[0]
    router_out = jnp.dot(routed, router, precision=lax.Precision.HIGHEST)
    normed_in = rms_scale(routed, gain_one).astype(jnp.bfloat16)
    packed = jnp.dot(normed_in, full_qkv, preferred_element_type=jnp.float32).astype(jnp.bfloat16)
    heads = packed.reshape(row_count, 3, HEADS, HEAD)
    allowed = (documents[:, None] == documents[None, :]) & (
        positions[None, :] <= positions[:, None]
    )
    scores = (
        jnp.einsum("qhd,khd->hqk", heads[:, 0], heads[:, 1], preferred_element_type=jnp.float32)
        * 0.125
    )
    scores = jnp.where(allowed[None], scores, -1000000000.0)
    row_max = jnp.max(scores, axis=-1, keepdims=True)
    log_total = row_max + jnp.log(jnp.sum(jnp.exp(scores - row_max), axis=-1, keepdims=True))
    prob_rows = jnp.exp(scores - log_total)
    prob_low = prob_rows.astype(jnp.bfloat16)
    attended = jnp.einsum("hqk,khd->qhd", prob_low, heads[:, 2], preferred_element_type=jnp.float32)
    attended = attended.reshape(row_count, D).astype(jnp.bfloat16)
    attn_out = jnp.dot(attended, full_out, preferred_element_type=jnp.float32)
    middle = routed + attn_out
    normed_mid = rms_scale(middle, gain_two).astype(jnp.bfloat16)
    up_in = jnp.dot(normed_mid, full_up, preferred_element_type=jnp.float32)
    activated = jax.nn.gelu(up_in).astype(jnp.bfloat16)
    mlp_out = jnp.dot(activated, full_down, preferred_element_type=jnp.float32)
    return (
        routed,
        router_out,
        normed_in,
        heads,
        prob_rows,
        prob_low,
        attended,
        attn_out,
        middle,
        normed_mid,
        up_in,
        activated,
        mlp_out,
    )


def general_device(
    hidden, cotangent, route_pos, route_doc, w_qkv, w_out, w_up, w_down, router, gain_one, gain_two
):
    positions = route_pos[0]
    documents = route_doc[0]
    live_mask = (documents < 2).astype(jnp.float32)[:, None]
    gathered = (
        lax.all_gather(w_qkv, "fsdp", axis=0, tiled=True),
        lax.all_gather(w_out, "fsdp", axis=0, tiled=True),
        lax.all_gather(w_up, "fsdp", axis=0, tiled=True),
        lax.all_gather(w_down, "fsdp", axis=0, tiled=True),
    )
    state = forward(hidden, positions, documents, gathered, router, gain_one, gain_two)
    attn_first = state[7]
    mlp_first = state[12]
    added = live_mask * state[1][:, None] * (attn_first + mlp_first)
    output = hidden.astype(jnp.float32).at[positions].add(added).astype(jnp.bfloat16)
    weights = (
        lax.all_gather(w_qkv, "fsdp", axis=0, tiled=True),
        lax.all_gather(w_out, "fsdp", axis=0, tiled=True),
        lax.all_gather(w_up, "fsdp", axis=0, tiled=True),
        lax.all_gather(w_down, "fsdp", axis=0, tiled=True),
    )
    state = forward(hidden, positions, documents, weights, router, gain_one, gain_two)
    full_qkv, full_out, full_up, full_down = weights
    (
        routed,
        router_out,
        normed_in,
        heads,
        prob_rows,
        prob_low,
        attended,
        attn_out,
        middle,
        normed_mid,
        up_in,
        activated,
        mlp_out,
    ) = state
    row_count = routed.shape[0]
    branch_out = attn_out + mlp_out
    grad_add = live_mask * cotangent[positions].astype(jnp.float32)
    grad_branch = grad_add * router_out[:, None]
    grad_score = jnp.sum(grad_add * branch_out, axis=-1)
    grad_mlp = grad_branch.astype(jnp.bfloat16)
    grad_down = jnp.dot(activated.T, grad_mlp, preferred_element_type=jnp.float32)
    grad_act = jnp.dot(grad_mlp, full_down.T, preferred_element_type=jnp.float32)
    _, gelu_pull = jax.vjp(jax.nn.gelu, up_in)
    grad_up_in = gelu_pull(grad_act)[0].astype(jnp.bfloat16)
    grad_up = jnp.dot(normed_mid.T, grad_up_in, preferred_element_type=jnp.float32)
    grad_norm_mid = jnp.dot(grad_up_in, full_up.T, preferred_element_type=jnp.float32)
    _, second_pull = jax.vjp(rms_scale, middle, gain_two)
    grad_middle, grad_gain_two = second_pull(grad_norm_mid)
    grad_attn = (grad_branch + grad_middle).astype(jnp.bfloat16)
    grad_out = jnp.dot(attended.T, grad_attn, preferred_element_type=jnp.float32)
    grad_attended = jnp.dot(grad_attn, full_out.T, preferred_element_type=jnp.float32).astype(
        jnp.bfloat16
    )
    grad_attended = grad_attended.reshape(row_count, HEADS, HEAD)
    grad_prob = jnp.einsum(
        "qhd,khd->hqk", grad_attended, heads[:, 2], preferred_element_type=jnp.float32
    )
    grad_value = jnp.einsum(
        "hqk,qhd->khd", prob_low, grad_attended, preferred_element_type=jnp.float32
    )
    row_dot = jnp.sum(grad_prob * prob_rows, axis=-1, keepdims=True)
    grad_scores = (prob_rows * (grad_prob - row_dot)).astype(jnp.bfloat16)
    grad_query = (
        jnp.einsum("hqk,khd->qhd", grad_scores, heads[:, 1], preferred_element_type=jnp.float32)
        * 0.125
    )
    grad_key = (
        jnp.einsum("hqk,qhd->khd", grad_scores, heads[:, 0], preferred_element_type=jnp.float32)
        * 0.125
    )
    grad_packed = jnp.stack([grad_query, grad_key, grad_value], axis=1).reshape(row_count, 3 * D)
    grad_packed = grad_packed.astype(jnp.bfloat16)
    grad_qkv = jnp.dot(normed_in.T, grad_packed, preferred_element_type=jnp.float32)
    grad_norm_in = jnp.dot(grad_packed, full_qkv.T, preferred_element_type=jnp.float32)
    _, first_pull = jax.vjp(rms_scale, routed, gain_one)
    grad_routed, grad_gain_one = first_pull(grad_norm_in)
    grad_routed = grad_routed + grad_middle + grad_score[:, None] * router[None, :]
    grad_router = jnp.dot(grad_score, routed, precision=lax.Precision.HIGHEST)
    grad_hidden = cotangent.astype(jnp.float32).at[positions].add(grad_routed).astype(jnp.bfloat16)
    shard_sums = (
        lax.psum_scatter(grad_qkv.astype(jnp.bfloat16), "fsdp", scatter_dimension=0, tiled=True),
        lax.psum_scatter(grad_out.astype(jnp.bfloat16), "fsdp", scatter_dimension=0, tiled=True),
        lax.psum_scatter(grad_up.astype(jnp.bfloat16), "fsdp", scatter_dimension=0, tiled=True),
        lax.psum_scatter(grad_down.astype(jnp.bfloat16), "fsdp", scatter_dimension=0, tiled=True),
    )
    final_sums = lax.psum((shard_sums[0], shard_sums[1], shard_sums[2], shard_sums[3]), "dp")
    small_sums = lax.psum((grad_router, grad_gain_one, grad_gain_two), ("dp", "fsdp"))
    return (
        output,
        grad_hidden,
        final_sums[0].astype(jnp.float32),
        final_sums[1].astype(jnp.float32),
        final_sums[2].astype(jnp.float32),
        final_sums[3].astype(jnp.float32),
        small_sums[0],
        small_sums[1],
        small_sums[2],
    )


MESH = pl.DeviceIdType.MESH
ANY = pl.ANY


def flip(index, stride):
    return index + stride - 2 * stride * ((index // stride) % 2)


def places():
    z = lax.axis_index("dp")
    f = lax.axis_index("fsdp")
    return z, f, flip(f, 1), flip(f, 2), flip(f, 4), flip(flip(f, 2), 4)


def greet(peers):
    barrier = pltpu.get_barrier_semaphore()
    for peer in peers:
        pl.semaphore_signal(barrier, inc=1, device_id=peer, device_id_type=MESH)
    pl.semaphore_wait(barrier, len(peers))


GATHER_KINDS = 13


ROOT = 0.7978845608028654
CUBE = 0.044715
EPSILON = 1e-06


def tile(i, size):
    return pl.ds(pl.multiple_of(i * size, size), size)


def each(count, fn):
    def step(i, carry):
        fn(i)
        return carry

    lax.fori_loop(0, count, step, 0)


def dot(left, right, dims=((1,), (0,))):
    return lax.dot_general(left, right, (dims, ((), ())), preferred_element_type=jnp.float32)


def inverse_size(values):
    return lax.rsqrt(jnp.mean(values * values, axis=-1, keepdims=True) + EPSILON)


def lane_half(shape):
    return lax.broadcasted_iota(jnp.int32, shape, 1) < HEAD


def head_probs(query, keys, allowed):
    scores = jnp.where(allowed, dot(query, keys, ((1,), (1,))) * 0.125, -1000000000.0)
    raised = jnp.exp(scores - jnp.max(scores, axis=-1, keepdims=True))
    return raised / jnp.sum(raised, axis=-1, keepdims=True)


def forward_kernel(*refs):
    shards = refs[0:4]
    hidden, cotangent, pos_col, pos_row, doc_col, doc_row, router, gain_one, gain_two = refs[4:13]
    outs = refs[13:30]
    fulls = refs[30:34]
    (tokens, cotokens, hit, routed, taken, normed_in, packed, attended, attn_out, middle) = refs[34:44]
    (normed_mid, slope, activated, grad_mlp, grad_branch, rows_out, score, gate) = refs[44:52]
    own_in, token_in, out_sem, send, recv = refs[52:57]
    z, f, core, along_x, along_y, across = places()
    pair = flip(z, 1)
    at_core, at_x, at_y, at_z = (z, core), (z, along_x), (z, along_y), (pair, f)
    greet((at_core, at_x, at_y, at_z))
    count = routed.shape[0]
    part = count // 4

    def rows_of(w, origin, start, size):
        rows = shards[w].shape[0]
        return pl.ds(pl.multiple_of(origin * rows + start, 16), size)

    def copy(w, kind, source, origin, start, size, peer):
        return pltpu.make_async_remote_copy(
            src_ref=source,
            dst_ref=fulls[w].at[rows_of(w, origin, start, size)],
            send_sem=send.at[w, kind],
            recv_sem=recv.at[w, kind],
            device_id=peer,
            device_id_type=MESH,
        )

    def own(w, kind, start, size, peer):
        source = shards[w].at[pl.ds(pl.multiple_of(start, 16), size)]
        return copy(w, kind, source, f, start, size, peer)

    def passed(w, kind, origin, start, size, peer):
        return copy(w, kind, fulls[w].at[rows_of(w, origin, start, size)], origin, start, size, peer)

    plan = []
    for w in range(4):
        rows = shards[w].shape[0]
        half = rows // 2
        even, odd = (z % 2) * half, (1 - z % 2) * half
        plan.append(
            [
                own(w, 0, even, half, at_x),
                own(w, 1, odd, half, at_y),
                own(w, 2, 0, rows, at_core),
                passed(w, 3, along_y, odd, half, at_x),
                passed(w, 4, along_x, even, half, at_y),
                passed(w, 5, along_x, even, half, at_z),
                passed(w, 6, along_y, odd, half, at_z),
                passed(w, 7, along_x, even, half, at_core),
                passed(w, 8, along_y, odd, half, at_core),
                passed(w, 9, across, odd, half, at_core),
                passed(w, 10, across, even, half, at_core),
                passed(w, 11, along_x, odd, half, at_core),
                passed(w, 12, along_y, even, half, at_core),
            ]
        )

    def first(w):
        for kind in (0, 1, 2):
            plan[w][kind].start()

    def second(w):
        plan[w][0].wait_recv()
        for kind in (5, 4, 7):
            plan[w][kind].start()
        plan[w][1].wait_recv()
        for kind in (6, 3, 8):
            plan[w][kind].start()

    def third(w):
        for kind, onward in ((3, 9), (4, 10), (5, 11), (6, 12)):
            plan[w][kind].wait_recv()
            plan[w][onward].start()

    def finish(w):
        loads[w].wait()
        for kind in (2,) + tuple(range(7, GATHER_KINDS)):
            plan[w][kind].wait_recv()
        put(w, fulls[w])

    def put(i, source):
        pltpu.make_async_copy(source, outs[i], out_sem.at[i]).start()

    def settle(i, source):
        pltpu.make_async_copy(source, outs[i], out_sem.at[i]).wait()

    loads = [
        pltpu.make_async_copy(
            shards[w], fulls[w].at[rows_of(w, f, 0, shards[w].shape[0])], own_in.at[w]
        )
        for w in range(4)
    ]
    token_loads = [
        pltpu.make_async_copy(hidden, tokens, token_in.at[0]),
        pltpu.make_async_copy(cotangent, cotokens, token_in.at[1]),
    ]
    first(0)
    first(1)
    for load in token_loads + loads:
        load.start()

    def mark(i):
        slots = lax.broadcasted_iota(jnp.int32, (part, hit.shape[1]), 1)
        hit[tile(i, part)] = (slots == pos_col[tile(i, part)]).astype(jnp.bfloat16)

    each(4, mark)

    def take(source, target):
        def columns(n):
            target[:, tile(n, 256)] = dot(hit[...], source[:, tile(n, 256)]).astype(target.dtype)

        each(D // 256, columns)

    token_loads[0].wait()
    take(tokens, routed)
    token_loads[1].wait()
    take(cotokens, taken)

    def open_rows(i):
        at = tile(i, part)
        rows = routed[at]
        normed_in[at] = (rows * inverse_size(rows) * gain_one[...]).astype(jnp.bfloat16)
        router_out = jnp.sum(rows * router[...], axis=-1, keepdims=True)
        gate_rows = jnp.where(doc_col[at] < 2, router_out, 0.0)
        gate[at] = jnp.broadcast_to(gate_rows, (part, 128))
        grad_rows = taken[at].astype(jnp.float32) * gate_rows
        grad_branch[at] = grad_rows
        grad_mlp[at] = grad_rows.astype(jnp.bfloat16)

    each(4, open_rows)
    for i, source in ((4, routed), (5, taken), (6, normed_in), (13, grad_mlp), (14, grad_branch)):
        put(i, source)
    second(0)
    first(2)
    second(1)
    first(3)
    third(0)
    finish(0)

    def pack(n):
        packed[:, tile(n, 512)] = dot(normed_in[...], fulls[0][:, tile(n, 512)]).astype(jnp.bfloat16)

    each(6, pack)
    put(7, packed)
    second(2)

    def attend(i):
        query, keys, values = (packed[:, tile(i + 8 * k, 128)] for k in range(3))
        allowed = (doc_col[...] == doc_row[...]) & (pos_row[...] <= pos_col[...])
        low = lane_half(query.shape)
        zero = jnp.zeros_like(query)
        mixed = [
            dot(head_probs(jnp.where(keep, query, zero), keys, allowed).astype(jnp.bfloat16), values)
            for keep in (low, ~low)
        ]
        attended[:, tile(i, 128)] = jnp.where(low, mixed[0], mixed[1]).astype(jnp.bfloat16)

    each(HEADS // 2, attend)
    put(8, attended)
    third(1)
    finish(1)

    def project(n):
        attn_out[:, tile(n, 256)] = dot(attended[...], fulls[1][:, tile(n, 256)])

    each(4, project)

    def middle_rows(i):
        at = tile(i, part)
        rows = routed[at] + attn_out[at]
        middle[at] = rows
        normed_mid[at] = (rows * inverse_size(rows) * gain_two[...]).astype(jnp.bfloat16)

    each(4, middle_rows)
    put(9, middle)
    put(10, normed_mid)
    second(3)
    third(2)
    finish(2)

    def raise_up(n):
        at = tile(n, 256)
        up = dot(normed_mid[...], fulls[2][:, at])
        square = up * up
        bend = jnp.tanh(ROOT * (up + CUBE * (square * up)))
        ahead = 0.5 * (1.0 + bend)
        activated[:, at] = (up * ahead).astype(jnp.bfloat16)
        slope[:, at] = ahead + 0.5 * up * (1.0 - bend * bend) * (ROOT * (1.0 + 3.0 * CUBE * square))

    each(16, raise_up)
    put(11, activated)
    put(12, slope)
    third(3)
    finish(3)

    def lower(n):
        at = tile(n, 256)
        attn_out[:, at] = attn_out[:, at] + dot(activated[...], fulls[3][:, at])

    each(4, lower)

    def close_rows(i):
        at = tile(i, part)
        branch = attn_out[at]
        rows_out[at] = (routed[at] + gate[at, 0:1] * branch).astype(jnp.bfloat16)
        grad_add = jnp.where(doc_col[at] < 2, taken[at].astype(jnp.float32), 0.0)
        total = jnp.sum(grad_add * branch, axis=-1, keepdims=True)
        score[at] = jnp.broadcast_to(total, (part, 128))

    each(4, close_rows)
    put(15, rows_out)
    put(16, score)
    kept = (routed, taken, normed_in, packed, attended, middle, normed_mid, activated, slope)
    for i, source in enumerate(tuple(fulls) + kept + (grad_mlp, grad_branch, rows_out, score)):
        settle(i, source)
    for w in range(4):
        for kind in range(GATHER_KINDS):
            plan[w][kind].wait_send()


def run_forward(weights, parts, hidden, cotangent, positions, documents, router, gain_one, gain_two):
    bf16, f32, dma = jnp.bfloat16, jnp.float32, pltpu.SemaphoreType.DMA
    count, wide = positions.shape[0], weights[2].shape[1]
    full = [((w.shape[0] * parts, w.shape[1]), w.dtype) for w in weights]
    row, head_row, wide_row = (count, D), (count, 3 * D), (count, wide)
    kept = [(row, f32), (row, bf16), (row, bf16), (head_row, bf16), (row, bf16), (row, f32)]
    kept += [(row, bf16), (wide_row, bf16), (wide_row, f32), (row, bf16), (row, f32), (row, bf16)]
    kept += [((count, 128), f32)]
    held = [(hidden.shape, bf16)] * 2 + [((count, hidden.shape[0]), bf16), (row, f32), (row, bf16)]
    held += [(row, bf16), (head_row, bf16), (row, bf16), (row, f32), (row, f32), (row, bf16)]
    held += [(wide_row, f32), (wide_row, bf16), (row, bf16), (row, f32), (row, bf16)]
    held += [((count, 128), f32)] * 2
    return pl.pallas_call(
        forward_kernel,
        out_shape=[jax.ShapeDtypeStruct(*each_one) for each_one in full + kept],
        in_specs=[pl.BlockSpec(memory_space=ANY)] * 6
        + [pl.BlockSpec(memory_space=pltpu.VMEM)] * 7,
        out_specs=[pl.BlockSpec(memory_space=ANY)] * 17,
        scratch_shapes=[pltpu.VMEM(*each_one) for each_one in full + held]
        + [dma((4,)), dma((2,)), dma((17,)), dma((4, GATHER_KINDS)), dma((4, GATHER_KINDS))],
        compiler_params=pltpu.CompilerParams(
            collective_id=1, has_side_effects=True, vmem_limit_bytes=60 * 1024 * 1024
        ),
        name="gather_and_forward",
    )(
        *weights,
        hidden,
        cotangent,
        positions[:, None],
        positions[None],
        documents[:, None],
        documents[None],
        router[None],
        gain_one[None],
        gain_two[None],
    )


CHUNKS = 24
LAGS = (1, 2, 3, 4, 5, 6)
LEFTS = 7
RIGHTS = 9
BLOCK = 128
WIDE = 512
FULL = 1024
LAST = 7


def left_of(t):
    return jnp.where(t < 8, t // 2, jnp.where(t < 16, 4, jnp.where(t < 22, 5, 6)))


def right_of(t):
    return jnp.where(t < 8, 0, t // 2 - 3)


def add_rows(target, sources, rows):
    def step(i, carry):
        at = pl.ds(pl.multiple_of(i * 16, 16), 16)
        total = sources[0][at].astype(jnp.float32)
        for source in sources[1:]:
            total = total + source[at].astype(jnp.float32)
        target[at] = total.astype(target.dtype)
        return carry

    lax.fori_loop(0, rows // 16, step, 0)


def reduce_kernel(*refs):
    activated, normed_mid, normed_in, attended, grad_mlp, grad_up_in, grad_packed, grad_attn = refs[:8]
    small, out_down, out_up, out_qkv, out_out, small_sums = refs[8:14]
    sums, stored = refs[35:37]
    (left, right, part, from_x, from_y, last_x, last_y, from_pair, from_far) = refs[14:23]
    small_sent, small_got = refs[23:25]
    (in_own, in_send, in_recv, rin_own, rin_send, rin_recv) = refs[25:31]
    send, recv, small_send, small_recv = refs[31:35]

    z, f, core, along_x, along_y, across = places()
    pair, far = flip(z, 1), 3 - z
    inner = (z == 1) | (z == 2)
    outer = (z == 0) | (z == 3)
    at_core, at_x, at_y = (z, core), (z, along_x), (z, along_y)
    at_pair, at_far = (pair, f), (far, f)
    greet((at_core, at_x, at_y, at_pair, at_far))

    rows = grad_mlp.shape[0]
    mine = pl.ds(pl.multiple_of((f % 2) * rows, rows), rows)
    half = BLOCK // 2
    top, bottom = pl.ds(0, half), pl.ds(half, half)

    def left_source(i):
        if i < 4:
            return activated, 4 * BLOCK, i * BLOCK
        return (normed_mid, normed_in, attended)[i - 4], BLOCK, 0

    def right_source(i):
        if i == 0:
            return grad_mlp, 0
        if i < 5:
            return grad_up_in, (i - 1) * FULL
        if i < 8:
            return grad_packed, (i - 5) * FULL
        return grad_attn, 0

    def spread(index):
        return (index, flip(index, 2), flip(index, 4), flip(flip(index, 2), 4))

    def left_copies(i):
        source, stride, offset = left_source(i)
        here, there = [], []
        for slot in range(4):
            target = left.at[i, mine, pl.ds(slot * BLOCK, BLOCK)]
            columns = [
                pl.ds(pl.multiple_of(spread(index)[slot] * stride + offset, BLOCK), BLOCK)
                for index in (f, core)
            ]
            here.append(
                pltpu.make_async_copy(source.at[:, columns[0]], target, in_own.at[i, slot])
            )
            there.append(
                pltpu.make_async_remote_copy(
                    src_ref=source.at[:, columns[1]],
                    dst_ref=target,
                    send_sem=in_send.at[i, slot],
                    recv_sem=in_recv.at[i, slot],
                    device_id=at_core,
                    device_id_type=MESH,
                )
            )
        return here + there

    def right_copies(i):
        source, offset = right_source(i)
        source = source.at[:, pl.ds(offset, FULL)]
        target = right.at[i, mine]
        return [
            pltpu.make_async_copy(source, target, rin_own.at[i]),
            pltpu.make_async_remote_copy(
                src_ref=source,
                dst_ref=target,
                send_sem=rin_send.at[i],
                recv_sem=rin_recv.at[i],
                device_id=at_core,
                device_id_type=MESH,
            ),
        ]

    lefts = [left_copies(i) for i in range(LEFTS)]
    rights = [right_copies(i) for i in range(RIGHTS)]
    new_left = {0: 0, 2: 1, 4: 2, 6: 3, 8: 4, 16: 5, 22: 6}
    new_right = {0: 0, 8: 1, 10: 2, 12: 3, 14: 4, 16: 5, 18: 6, 20: 7, 22: 8}
    for t in range(CHUNKS):
        for copy in lefts[new_left[t]] if t in new_left else ():
            copy.start()
        for copy in rights[new_right[t]] if t in new_right else ():
            copy.start()

    def remote(t, kind, source, target, peer):
        return pltpu.make_async_remote_copy(
            src_ref=source,
            dst_ref=target,
            send_sem=send.at[t, kind],
            recv_sem=recv.at[t, kind],
            device_id=peer,
            device_id_type=MESH,
        )

    def moved(t, kind):
        source, target, peer = (
            lambda: (part.at[t, 1, top], from_x.at[t, 0], at_x),
            lambda: (part.at[t, 3, top], from_x.at[t, 1], at_x),
            lambda: (part.at[t, 2, bottom], from_y.at[t, 0], at_y),
            lambda: (part.at[t, 3, bottom], from_y.at[t, 1], at_y),
            lambda: (part.at[t, 1, bottom], last_x.at[t], at_x),
            lambda: (part.at[t, 2, top], last_y.at[t], at_y),
            lambda: (part.at[t, 0], from_pair.at[t], at_pair),
            lambda: (part.at[t, 0], from_far.at[t], at_far),
            lambda: (sums.at[t], sums.at[t], at_pair),
        )[kind]()
        return remote(t, kind, source, target, peer)

    def stage_product(t):
        lhs = left[left_of(t)]
        for column in range(0, WIDE, 256):
            block = lax.dot_general(
                lhs,
                right[right_of(t), :, pl.ds(pl.multiple_of((t % 2) * WIDE + column, 256), 256)],
                (((0,), (0,)), ((), ())),
                preferred_element_type=jnp.float32,
            ).astype(jnp.bfloat16)
            for slot in range(4):
                part[t, slot, :, column : column + 256] = block[slot * BLOCK : (slot + 1) * BLOCK]
        for kind in (1, 3, 0, 2):
            moved(t, kind).start()

    def stage_turn(t):
        moved(t, 1).wait_recv()
        add_rows(part.at[t, 2, top], (part.at[t, 2, top], from_x.at[t, 1]), half)
        moved(t, 5).start()
        moved(t, 3).wait_recv()
        add_rows(part.at[t, 1, bottom], (part.at[t, 1, bottom], from_y.at[t, 1]), half)
        moved(t, 4).start()

    def stage_plane(t):
        moved(t, 0).wait_recv()
        moved(t, 5).wait_recv()
        add_rows(part.at[t, 0, top], (part.at[t, 0, top], from_x.at[t, 0], last_y.at[t]), half)
        moved(t, 2).wait_recv()
        moved(t, 4).wait_recv()
        add_rows(
            part.at[t, 0, bottom], (part.at[t, 0, bottom], from_y.at[t, 0], last_x.at[t]), half
        )

        @pl.when(outer)
        def _():
            moved(t, 6).start()

    def stage_pair(t):
        @pl.when(inner)
        def _():
            moved(t, 6).wait_recv()
            add_rows(part.at[t, 0], (part.at[t, 0], from_pair.at[t]), BLOCK)
            moved(t, 7).start()

    def stage_far(t):
        @pl.when(inner)
        def _():
            moved(t, 7).wait_recv()
            add_rows(sums.at[t], (part.at[t, 0], from_far.at[t]), BLOCK)
            moved(t, 8).start()

    def stage_end(t):
        @pl.when(inner)
        def _():
            moved(t, 7).wait_send()
            moved(t, 8).wait_send()

        @pl.when(outer)
        def _():
            moved(t, 6).wait_send()
            moved(t, 8).wait_recv()

        for kind in range(6):
            moved(t, kind).wait_send()

        store(t, True)

    def store(t, begin):
        for low, high, target in (
            (0, 8, lambda i: out_down.at[pl.ds(pl.multiple_of(i // 2 * BLOCK, BLOCK), BLOCK), columns(i % 2)]),
            (8, 16, lambda i: out_up.at[:, columns(i)]),
            (16, 22, lambda i: out_qkv.at[:, columns(i)]),
            (22, 24, lambda i: out_out.at[:, columns(i)]),
        ):

            @pl.when((t >= low) & (t < high))
            def _(low=low, target=target):
                copy = pltpu.make_async_copy(sums.at[t], target(t - low), stored.at[t])
                copy.start() if begin else copy.wait()

    def columns(i):
        return pl.ds(pl.multiple_of(i * WIDE, WIDE), WIDE)

    def stage_stored(t):
        store(t, False)

    peers = (at_core, at_x, at_y, at_pair, at_far)

    def small_copy(j):
        return pltpu.make_async_remote_copy(
            src_ref=small_sent.at[j],
            dst_ref=small_got.at[j],
            send_sem=small_send.at[j],
            recv_sem=small_recv.at[j],
            device_id=peers[j],
            device_id_type=MESH,
        )

    small_sent[0] = small[...]
    small_copy(0).start()
    stages = (stage_turn, stage_plane, stage_pair, stage_far, stage_end, stage_stored)

    def tick(t, carry):
        for when, i in new_left.items():

            @pl.when(t == when)
            def _(i=i):
                for copy in lefts[i]:
                    copy.wait()

        for when, i in new_right.items():

            @pl.when(t == when)
            def _(i=i):
                for copy in rights[i]:
                    copy.wait()

        @pl.when(t < CHUNKS)
        def _():
            stage_product(t)

        for lag, stage in zip(LAGS, stages):

            @pl.when((t >= lag) & (t < CHUNKS + lag))
            def _(lag=lag, stage=stage):
                stage(t - lag)

        for j in range(5):

            @pl.when(t == j)
            def _(j=j):
                small_copy(j).wait()
                total = small_sent[j] + small_got[j]
                if j < 4:
                    small_sent[j + 1] = total
                    small_copy(j + 1).start()
                else:
                    small_sums[...] = total

        return carry

    lax.fori_loop(0, CHUNKS + LAGS[-1], tick, 0)


def reduce_gradients(lefts, rights, small):
    rows = lefts[0].shape[0]
    bf16, dma = jnp.bfloat16, pltpu.SemaphoreType.DMA
    return pl.pallas_call(
        reduce_kernel,
        out_shape=[
            jax.ShapeDtypeStruct((4 * BLOCK, FULL), bf16),
            jax.ShapeDtypeStruct((BLOCK, 4 * FULL), bf16),
            jax.ShapeDtypeStruct((BLOCK, 3 * FULL), bf16),
            jax.ShapeDtypeStruct((BLOCK, FULL), bf16),
            jax.ShapeDtypeStruct(small.shape, jnp.float32),
        ],
        in_specs=[pl.BlockSpec(memory_space=ANY)] * 8 + [pl.BlockSpec(memory_space=pltpu.VMEM)],
        out_specs=[pl.BlockSpec(memory_space=ANY)] * 4 + [pl.BlockSpec(memory_space=pltpu.VMEM)],
        scratch_shapes=[
            pltpu.VMEM((LEFTS, 2 * rows, 4 * BLOCK), bf16),
            pltpu.VMEM((RIGHTS, 2 * rows, FULL), bf16),
            pltpu.VMEM((CHUNKS, 4, BLOCK, WIDE), bf16),
            pltpu.VMEM((CHUNKS, 2, BLOCK // 2, WIDE), bf16),
            pltpu.VMEM((CHUNKS, 2, BLOCK // 2, WIDE), bf16),
            pltpu.VMEM((CHUNKS, BLOCK // 2, WIDE), bf16),
            pltpu.VMEM((CHUNKS, BLOCK // 2, WIDE), bf16),
            pltpu.VMEM((CHUNKS, BLOCK, WIDE), bf16),
            pltpu.VMEM((CHUNKS, BLOCK, WIDE), bf16),
            pltpu.VMEM((5,) + small.shape, jnp.float32),
            pltpu.VMEM((5,) + small.shape, jnp.float32),
            dma((LEFTS, 4)),
            dma((LEFTS, 4)),
            dma((LEFTS, 4)),
            dma((RIGHTS,)),
            dma((RIGHTS,)),
            dma((RIGHTS,)),
            dma((CHUNKS, 9)),
            dma((CHUNKS, 9)),
            dma((5,)),
            dma((5,)),
            pltpu.VMEM((CHUNKS, BLOCK, WIDE), bf16),
            dma((CHUNKS,)),
        ],
        compiler_params=pltpu.CompilerParams(
            collective_id=2, has_side_effects=True, vmem_limit_bytes=60 * 1024 * 1024
        ),
        name="reduce_gradients",
    )(*lefts, *rights, small)


def put_rows(tokens, rows, positions):
    hit = lax.broadcasted_iota(jnp.int32, (tokens.shape[0], positions.shape[0]), 0) == positions[None]
    moved = jnp.dot(hit.astype(jnp.bfloat16), rows, preferred_element_type=jnp.float32)
    return jnp.where(jnp.any(hit, axis=1, keepdims=True), moved.astype(jnp.bfloat16), tokens)


def per_device(
    hidden, cotangent, route_pos, route_doc, w_qkv, w_out, w_up, w_down, router, gain_one, gain_two
):
    positions = route_pos[0]
    documents = route_doc[0]
    (
        full_qkv,
        full_out,
        full_up,
        full_down,
        routed,
        taken,
        normed_in,
        packed,
        attended,
        middle,
        normed_mid,
        activated,
        slope,
        grad_mlp,
        grad_branch,
        rows_out,
        score,
    ) = run_forward(
        (w_qkv, w_out, w_up, w_down),
        8,
        hidden,
        cotangent,
        positions,
        documents,
        router,
        gain_one,
        gain_two,
    )
    row_count = routed.shape[0]
    output = put_rows(hidden, rows_out, positions)
    grad_score = score[:, 0]
    heads = packed.reshape(row_count, 3, HEADS, HEAD)
    allowed = (documents[:, None] == documents[None, :]) & (
        positions[None, :] <= positions[:, None]
    )
    scores = (
        jnp.einsum("qhd,khd->hqk", heads[:, 0], heads[:, 1], preferred_element_type=jnp.float32)
        * 0.125
    )
    prob_rows = jax.nn.softmax(jnp.where(allowed[None], scores, -1000000000.0), axis=-1)
    prob_low = prob_rows.astype(jnp.bfloat16)
    grad_act = jnp.dot(grad_mlp, full_down.T, preferred_element_type=jnp.float32)
    grad_up_in = (grad_act * slope).astype(jnp.bfloat16)
    grad_norm_mid = jnp.dot(grad_up_in, full_up.T, preferred_element_type=jnp.float32)
    _, second_pull = jax.vjp(rms_scale, middle, gain_two)
    grad_middle, grad_gain_two = second_pull(grad_norm_mid)
    grad_attn = (grad_branch + grad_middle).astype(jnp.bfloat16)
    grad_attended = jnp.dot(grad_attn, full_out.T, preferred_element_type=jnp.float32).astype(
        jnp.bfloat16
    )
    grad_attended = grad_attended.reshape(row_count, HEADS, HEAD)
    grad_prob = jnp.einsum(
        "qhd,khd->hqk", grad_attended, heads[:, 2], preferred_element_type=jnp.float32
    )
    grad_value = jnp.einsum(
        "hqk,qhd->khd", prob_low, grad_attended, preferred_element_type=jnp.float32
    )
    row_dot = jnp.sum(grad_prob * prob_rows, axis=-1, keepdims=True)
    grad_scores = (prob_rows * (grad_prob - row_dot)).astype(jnp.bfloat16)
    grad_query = (
        jnp.einsum("hqk,khd->qhd", grad_scores, heads[:, 1], preferred_element_type=jnp.float32)
        * 0.125
    )
    grad_key = (
        jnp.einsum("hqk,qhd->khd", grad_scores, heads[:, 0], preferred_element_type=jnp.float32)
        * 0.125
    )
    grad_packed = jnp.stack([grad_query, grad_key, grad_value], axis=1).reshape(row_count, 3 * D)
    grad_packed = grad_packed.astype(jnp.bfloat16)
    grad_norm_in = jnp.dot(grad_packed, full_qkv.T, preferred_element_type=jnp.float32)
    _, first_pull = jax.vjp(rms_scale, routed, gain_one)
    grad_routed, grad_gain_one = first_pull(grad_norm_in)
    grad_routed = grad_routed + grad_middle + grad_score[:, None] * router[None, :]
    grad_router = jnp.dot(grad_score, routed, precision=lax.Precision.HIGHEST)
    grad_hidden = put_rows(cotangent, (taken.astype(jnp.float32) + grad_routed).astype(jnp.bfloat16), positions)
    small = jnp.stack([grad_router, grad_gain_one, grad_gain_two] + [jnp.zeros_like(grad_router)] * 5)
    *sums, small_sums = reduce_gradients(
        (activated, normed_mid, normed_in, attended),
        (grad_mlp, grad_up_in, grad_packed, grad_attn),
        small,
    )
    sum_down, sum_up, sum_qkv, sum_out = (total.astype(jnp.float32) for total in sums)
    return (
        output,
        grad_hidden,
        sum_qkv,
        sum_out,
        sum_up,
        sum_down,
        small_sums[0],
        small_sums[1],
        small_sums[2],
    )


def solution(mesh):
    paired = dict(mesh.shape) == {"dp": 4, "fsdp": 8}
    tokens, weights = P(("dp", "fsdp"), None), P("fsdp", None)
    return jax.shard_map(
        per_device if paired else general_device,
        mesh=mesh,
        in_specs=(tokens,) * 4 + (weights,) * 4 + (P(),) * 3,
        out_specs=(tokens,) * 2 + (weights,) * 4 + (P(),) * 3,
        check_vma=False,
    )
```

```python
import functools

import jax
import jax.numpy as jnp
from jax import lax
from jax.experimental import pallas as pl
from jax.experimental.pallas import tpu as pltpu
from jax.sharding import PartitionSpec as P

D = 1024
HEADS = 16
HEAD = 64


EPS = 1e-06


def rms_scale(values, gain_vec):
    return values * lax.rsqrt(jnp.mean(values * values, axis=-1, keepdims=True) + EPS) * gain_vec


def forward(tokens, positions, documents, weights, router, gain_one, gain_two):
    full_qkv, full_out, full_up, full_down = weights
    routed = tokens[positions].astype(jnp.float32)
    row_count = routed.shape[0]
    router_out = jnp.dot(routed, router, precision=lax.Precision.HIGHEST)
    normed_in = rms_scale(routed, gain_one).astype(jnp.bfloat16)
    packed = jnp.dot(normed_in, full_qkv, preferred_element_type=jnp.float32).astype(jnp.bfloat16)
    heads = packed.reshape(row_count, 3, HEADS, HEAD)
    allowed = (documents[:, None] == documents[None, :]) & (
        positions[None, :] <= positions[:, None]
    )
    scores = (
        jnp.einsum("qhd,khd->hqk", heads[:, 0], heads[:, 1], preferred_element_type=jnp.float32)
        * 0.125
    )
    scores = jnp.where(allowed[None], scores, -1000000000.0)
    row_max = jnp.max(scores, axis=-1, keepdims=True)
    log_total = row_max + jnp.log(jnp.sum(jnp.exp(scores - row_max), axis=-1, keepdims=True))
    prob_rows = jnp.exp(scores - log_total)
    prob_low = prob_rows.astype(jnp.bfloat16)
    attended = jnp.einsum("hqk,khd->qhd", prob_low, heads[:, 2], preferred_element_type=jnp.float32)
    attended = attended.reshape(row_count, D).astype(jnp.bfloat16)
    attn_out = jnp.dot(attended, full_out, preferred_element_type=jnp.float32)
    middle = routed + attn_out
    normed_mid = rms_scale(middle, gain_two).astype(jnp.bfloat16)
    up_in = jnp.dot(normed_mid, full_up, preferred_element_type=jnp.float32)
    activated = jax.nn.gelu(up_in).astype(jnp.bfloat16)
    mlp_out = jnp.dot(activated, full_down, preferred_element_type=jnp.float32)
    return (
        routed,
        router_out,
        normed_in,
        heads,
        prob_rows,
        prob_low,
        attended,
        attn_out,
        middle,
        normed_mid,
        up_in,
        activated,
        mlp_out,
    )


def general_device(
    hidden, cotangent, route_pos, route_doc, w_qkv, w_out, w_up, w_down, router, gain_one, gain_two
):
    positions = route_pos[0]
    documents = route_doc[0]
    live_mask = (documents < 2).astype(jnp.float32)[:, None]
    gathered = (
        lax.all_gather(w_qkv, "fsdp", axis=0, tiled=True),
        lax.all_gather(w_out, "fsdp", axis=0, tiled=True),
        lax.all_gather(w_up, "fsdp", axis=0, tiled=True),
        lax.all_gather(w_down, "fsdp", axis=0, tiled=True),
    )
    state = forward(hidden, positions, documents, gathered, router, gain_one, gain_two)
    attn_first = state[7]
    mlp_first = state[12]
    added = live_mask * state[1][:, None] * (attn_first + mlp_first)
    output = hidden.astype(jnp.float32).at[positions].add(added).astype(jnp.bfloat16)
    weights = (
        lax.all_gather(w_qkv, "fsdp", axis=0, tiled=True),
        lax.all_gather(w_out, "fsdp", axis=0, tiled=True),
        lax.all_gather(w_up, "fsdp", axis=0, tiled=True),
        lax.all_gather(w_down, "fsdp", axis=0, tiled=True),
    )
    state = forward(hidden, positions, documents, weights, router, gain_one, gain_two)
    full_qkv, full_out, full_up, full_down = weights
    (
        routed,
        router_out,
        normed_in,
        heads,
        prob_rows,
        prob_low,
        attended,
        attn_out,
        middle,
        normed_mid,
        up_in,
        activated,
        mlp_out,
    ) = state
    row_count = routed.shape[0]
    branch_out = attn_out + mlp_out
    grad_add = live_mask * cotangent[positions].astype(jnp.float32)
    grad_branch = grad_add * router_out[:, None]
    grad_score = jnp.sum(grad_add * branch_out, axis=-1)
    grad_mlp = grad_branch.astype(jnp.bfloat16)
    grad_down = jnp.dot(activated.T, grad_mlp, preferred_element_type=jnp.float32)
    grad_act = jnp.dot(grad_mlp, full_down.T, preferred_element_type=jnp.float32)
    _, gelu_pull = jax.vjp(jax.nn.gelu, up_in)
    grad_up_in = gelu_pull(grad_act)[0].astype(jnp.bfloat16)
    grad_up = jnp.dot(normed_mid.T, grad_up_in, preferred_element_type=jnp.float32)
    grad_norm_mid = jnp.dot(grad_up_in, full_up.T, preferred_element_type=jnp.float32)
    _, second_pull = jax.vjp(rms_scale, middle, gain_two)
    grad_middle, grad_gain_two = second_pull(grad_norm_mid)
    grad_attn = (grad_branch + grad_middle).astype(jnp.bfloat16)
    grad_out = jnp.dot(attended.T, grad_attn, preferred_element_type=jnp.float32)
    grad_attended = jnp.dot(grad_attn, full_out.T, preferred_element_type=jnp.float32).astype(
        jnp.bfloat16
    )
    grad_attended = grad_attended.reshape(row_count, HEADS, HEAD)
    grad_prob = jnp.einsum(
        "qhd,khd->hqk", grad_attended, heads[:, 2], preferred_element_type=jnp.float32
    )
    grad_value = jnp.einsum(
        "hqk,qhd->khd", prob_low, grad_attended, preferred_element_type=jnp.float32
    )
    row_dot = jnp.sum(grad_prob * prob_rows, axis=-1, keepdims=True)
    grad_scores = (prob_rows * (grad_prob - row_dot)).astype(jnp.bfloat16)
    grad_query = (
        jnp.einsum("hqk,khd->qhd", grad_scores, heads[:, 1], preferred_element_type=jnp.float32)
        * 0.125
    )
    grad_key = (
        jnp.einsum("hqk,qhd->khd", grad_scores, heads[:, 0], preferred_element_type=jnp.float32)
        * 0.125
    )
    grad_packed = jnp.stack([grad_query, grad_key, grad_value], axis=1).reshape(row_count, 3 * D)
    grad_packed = grad_packed.astype(jnp.bfloat16)
    grad_qkv = jnp.dot(normed_in.T, grad_packed, preferred_element_type=jnp.float32)
    grad_norm_in = jnp.dot(grad_packed, full_qkv.T, preferred_element_type=jnp.float32)
    _, first_pull = jax.vjp(rms_scale, routed, gain_one)
    grad_routed, grad_gain_one = first_pull(grad_norm_in)
    grad_routed = grad_routed + grad_middle + grad_score[:, None] * router[None, :]
    grad_router = jnp.dot(grad_score, routed, precision=lax.Precision.HIGHEST)
    grad_hidden = cotangent.astype(jnp.float32).at[positions].add(grad_routed).astype(jnp.bfloat16)
    shard_sums = (
        lax.psum_scatter(grad_qkv.astype(jnp.bfloat16), "fsdp", scatter_dimension=0, tiled=True),
        lax.psum_scatter(grad_out.astype(jnp.bfloat16), "fsdp", scatter_dimension=0, tiled=True),
        lax.psum_scatter(grad_up.astype(jnp.bfloat16), "fsdp", scatter_dimension=0, tiled=True),
        lax.psum_scatter(grad_down.astype(jnp.bfloat16), "fsdp", scatter_dimension=0, tiled=True),
    )
    final_sums = lax.psum((shard_sums[0], shard_sums[1], shard_sums[2], shard_sums[3]), "dp")
    small_sums = lax.psum((grad_router, grad_gain_one, grad_gain_two), ("dp", "fsdp"))
    return (
        output,
        grad_hidden,
        final_sums[0].astype(jnp.float32),
        final_sums[1].astype(jnp.float32),
        final_sums[2].astype(jnp.float32),
        final_sums[3].astype(jnp.float32),
        small_sums[0],
        small_sums[1],
        small_sums[2],
    )


MESH = pl.DeviceIdType.MESH
ANY = pl.ANY


def flip(index, stride):
    return index + stride - 2 * stride * ((index // stride) % 2)


def places():
    z = lax.axis_index("dp")
    f = lax.axis_index("fsdp")
    return z, f, flip(f, 1), flip(f, 2), flip(f, 4), flip(flip(f, 2), 4)


def greet(peers):
    barrier = pltpu.get_barrier_semaphore()
    for peer in peers:
        pl.semaphore_signal(barrier, inc=1, device_id=peer, device_id_type=MESH)
    pl.semaphore_wait(barrier, len(peers))


GATHER_KINDS = 13


ROOT = 0.7978845608028654
CUBE = 0.044715
EPSILON = 1e-06


def tile(i, size):
    return pl.ds(pl.multiple_of(i * size, size), size)


def each(count, fn):
    def step(i, carry):
        fn(i)
        return carry

    lax.fori_loop(0, count, step, 0)


def dot(left, right, dims=((1,), (0,))):
    return lax.dot_general(left, right, (dims, ((), ())), preferred_element_type=jnp.float32)


def inverse_size(values):
    return lax.rsqrt(jnp.mean(values * values, axis=-1, keepdims=True) + EPSILON)


def lane_half(shape):
    return lax.broadcasted_iota(jnp.int32, shape, 1) < HEAD


def head_probs(query, keys, allowed):
    scores = jnp.where(allowed, dot(query, keys, ((1,), (1,))) * 0.125, -1000000000.0)
    raised = jnp.exp(scores - jnp.max(scores, axis=-1, keepdims=True))
    return raised / jnp.sum(raised, axis=-1, keepdims=True)


def forward_kernel(*refs):
    shards = refs[0:4]
    hidden, cotangent, pos_col, pos_row, doc_col, doc_row, router, gain_one, gain_two = refs[4:13]
    outs = refs[13:30]
    fulls = refs[30:34]
    (tokens, cotokens, hit, routed, taken, normed_in, packed, attended, attn_out, middle) = refs[34:44]
    (normed_mid, slope, activated, grad_mlp, grad_branch, rows_out, score, gate) = refs[44:52]
    own_in, token_in, out_sem, send, recv = refs[52:57]
    z, f, core, along_x, along_y, across = places()
    pair = flip(z, 1)
    at_core, at_x, at_y, at_z = (z, core), (z, along_x), (z, along_y), (pair, f)
    greet((at_core, at_x, at_y, at_z))
    count = routed.shape[0]
    part = count // 4

    def rows_of(w, origin, start, size):
        rows = shards[w].shape[0]
        return pl.ds(pl.multiple_of(origin * rows + start, 16), size)

    def copy(w, kind, source, origin, start, size, peer):
        return pltpu.make_async_remote_copy(
            src_ref=source,
            dst_ref=fulls[w].at[rows_of(w, origin, start, size)],
            send_sem=send.at[w, kind],
            recv_sem=recv.at[w, kind],
            device_id=peer,
            device_id_type=MESH,
        )

    def own(w, kind, start, size, peer):
        source = shards[w].at[pl.ds(pl.multiple_of(start, 16), size)]
        return copy(w, kind, source, f, start, size, peer)

    def passed(w, kind, origin, start, size, peer):
        return copy(w, kind, fulls[w].at[rows_of(w, origin, start, size)], origin, start, size, peer)

    plan = []
    for w in range(4):
        rows = shards[w].shape[0]
        half = rows // 2
        even, odd = (z % 2) * half, (1 - z % 2) * half
        plan.append(
            [
                own(w, 0, even, half, at_x),
                own(w, 1, odd, half, at_y),
                own(w, 2, 0, rows, at_core),
                passed(w, 3, along_y, odd, half, at_x),
                passed(w, 4, along_x, even, half, at_y),
                passed(w, 5, along_x, even, half, at_z),
                passed(w, 6, along_y, odd, half, at_z),
                passed(w, 7, along_x, even, half, at_core),
                passed(w, 8, along_y, odd, half, at_core),
                passed(w, 9, across, odd, half, at_core),
                passed(w, 10, across, even, half, at_core),
                passed(w, 11, along_x, odd, half, at_core),
                passed(w, 12, along_y, even, half, at_core),
            ]
        )

    def first(w):
        for kind in (0, 1, 2):
            plan[w][kind].start()

    def second(w):
        plan[w][0].wait_recv()
        for kind in (5, 4, 7):
            plan[w][kind].start()
        plan[w][1].wait_recv()
        for kind in (6, 3, 8):
            plan[w][kind].start()

    def third(w):
        for kind, onward in ((3, 9), (4, 10), (5, 11), (6, 12)):
            plan[w][kind].wait_recv()
            plan[w][onward].start()

    def finish(w):
        loads[w].wait()
        for kind in (2,) + tuple(range(7, GATHER_KINDS)):
            plan[w][kind].wait_recv()
        put(w, fulls[w])

    def put(i, source):
        pltpu.make_async_copy(source, outs[i], out_sem.at[i]).start()

    def settle(i, source):
        pltpu.make_async_copy(source, outs[i], out_sem.at[i]).wait()

    loads = [
        pltpu.make_async_copy(
            shards[w], fulls[w].at[rows_of(w, f, 0, shards[w].shape[0])], own_in.at[w]
        )
        for w in range(4)
    ]
    token_loads = [
        pltpu.make_async_copy(hidden, tokens, token_in.at[0]),
        pltpu.make_async_copy(cotangent, cotokens, token_in.at[1]),
    ]
    first(0)
    first(1)
    for load in token_loads + loads:
        load.start()

    def mark(i):
        slots = lax.broadcasted_iota(jnp.int32, (part, hit.shape[1]), 1)
        hit[tile(i, part)] = (slots == pos_col[tile(i, part)]).astype(jnp.bfloat16)

    each(4, mark)

    def take(source, target):
        def columns(n):
            target[:, tile(n, 256)] = dot(hit[...], source[:, tile(n, 256)]).astype(target.dtype)

        each(D // 256, columns)

    token_loads[0].wait()
    take(tokens, routed)
    token_loads[1].wait()
    take(cotokens, taken)

    def open_rows(i):
        at = tile(i, part)
        rows = routed[at]
        normed_in[at] = (rows * inverse_size(rows) * gain_one[...]).astype(jnp.bfloat16)
        router_out = jnp.sum(rows * router[...], axis=-1, keepdims=True)
        gate_rows = jnp.where(doc_col[at] < 2, router_out, 0.0)
        gate[at] = jnp.broadcast_to(gate_rows, (part, 128))
        grad_rows = taken[at].astype(jnp.float32) * gate_rows
        grad_branch[at] = grad_rows
        grad_mlp[at] = grad_rows.astype(jnp.bfloat16)

    each(4, open_rows)
    for i, source in ((4, routed), (5, taken), (6, normed_in), (13, grad_mlp), (14, grad_branch)):
        put(i, source)
    second(0)
    first(2)
    second(1)
    first(3)
    third(0)
    finish(0)

    def pack(n):
        packed[:, tile(n, 512)] = dot(normed_in[...], fulls[0][:, tile(n, 512)]).astype(jnp.bfloat16)

    each(6, pack)
    put(7, packed)
    second(2)

    def attend(i):
        query, keys, values = (packed[:, tile(i + 8 * k, 128)] for k in range(3))
        allowed = (doc_col[...] == doc_row[...]) & (pos_row[...] <= pos_col[...])
        low = lane_half(query.shape)
        zero = jnp.zeros_like(query)
        mixed = [
            dot(head_probs(jnp.where(keep, query, zero), keys, allowed).astype(jnp.bfloat16), values)
            for keep in (low, ~low)
        ]
        attended[:, tile(i, 128)] = jnp.where(low, mixed[0], mixed[1]).astype(jnp.bfloat16)

    each(HEADS // 2, attend)
    put(8, attended)
    third(1)
    finish(1)

    def project(n):
        attn_out[:, tile(n, 256)] = dot(attended[...], fulls[1][:, tile(n, 256)])

    each(4, project)

    def middle_rows(i):
        at = tile(i, part)
        rows = routed[at] + attn_out[at]
        middle[at] = rows
        normed_mid[at] = (rows * inverse_size(rows) * gain_two[...]).astype(jnp.bfloat16)

    each(4, middle_rows)
    put(9, middle)
    put(10, normed_mid)
    second(3)
    third(2)
    finish(2)

    def raise_up(n):
        at = tile(n, 256)
        up = dot(normed_mid[...], fulls[2][:, at])
        square = up * up
        bend = jnp.tanh(ROOT * (up + CUBE * (square * up)))
        ahead = 0.5 * (1.0 + bend)
        activated[:, at] = (up * ahead).astype(jnp.bfloat16)
        slope[:, at] = ahead + 0.5 * up * (1.0 - bend * bend) * (ROOT * (1.0 + 3.0 * CUBE * square))

    each(16, raise_up)
    put(11, activated)
    put(12, slope)
    third(3)
    finish(3)

    def lower(n):
        at = tile(n, 256)
        attn_out[:, at] = attn_out[:, at] + dot(activated[...], fulls[3][:, at])

    each(4, lower)

    def close_rows(i):
        at = tile(i, part)
        branch = attn_out[at]
        rows_out[at] = (routed[at] + gate[at, 0:1] * branch).astype(jnp.bfloat16)
        grad_add = jnp.where(doc_col[at] < 2, taken[at].astype(jnp.float32), 0.0)
        total = jnp.sum(grad_add * branch, axis=-1, keepdims=True)
        score[at] = jnp.broadcast_to(total, (part, 128))

    each(4, close_rows)
    put(15, rows_out)
    put(16, score)
    kept = (routed, taken, normed_in, packed, attended, middle, normed_mid, activated, slope)
    for i, source in enumerate(tuple(fulls) + kept + (grad_mlp, grad_branch, rows_out, score)):
        settle(i, source)
    for w in range(4):
        for kind in range(GATHER_KINDS):
            plan[w][kind].wait_send()


def run_forward(weights, parts, hidden, cotangent, positions, documents, router, gain_one, gain_two):
    bf16, f32, dma = jnp.bfloat16, jnp.float32, pltpu.SemaphoreType.DMA
    count, wide = positions.shape[0], weights[2].shape[1]
    full = [((w.shape[0] * parts, w.shape[1]), w.dtype) for w in weights]
    row, head_row, wide_row = (count, D), (count, 3 * D), (count, wide)
    kept = [(row, f32), (row, bf16), (row, bf16), (head_row, bf16), (row, bf16), (row, f32)]
    kept += [(row, bf16), (wide_row, bf16), (wide_row, f32), (row, bf16), (row, f32), (row, bf16)]
    kept += [((count, 128), f32)]
    held = [(hidden.shape, bf16)] * 2 + [((count, hidden.shape[0]), bf16), (row, f32), (row, bf16)]
    held += [(row, bf16), (head_row, bf16), (row, bf16), (row, f32), (row, f32), (row, bf16)]
    held += [(wide_row, f32), (wide_row, bf16), (row, bf16), (row, f32), (row, bf16)]
    held += [((count, 128), f32)] * 2
    return pl.pallas_call(
        forward_kernel,
        out_shape=[jax.ShapeDtypeStruct(*each_one) for each_one in full + kept],
        in_specs=[pl.BlockSpec(memory_space=ANY)] * 6
        + [pl.BlockSpec(memory_space=pltpu.VMEM)] * 7,
        out_specs=[pl.BlockSpec(memory_space=ANY)] * 17,
        scratch_shapes=[pltpu.VMEM(*each_one) for each_one in full + held]
        + [dma((4,)), dma((2,)), dma((17,)), dma((4, GATHER_KINDS)), dma((4, GATHER_KINDS))],
        compiler_params=pltpu.CompilerParams(
            collective_id=1, has_side_effects=True, vmem_limit_bytes=60 * 1024 * 1024
        ),
        name="gather_and_forward",
    )(
        *weights,
        hidden,
        cotangent,
        positions[:, None],
        positions[None],
        documents[:, None],
        documents[None],
        router[None],
        gain_one[None],
        gain_two[None],
    )


CHUNKS = 24
LAGS = (1, 2, 3, 4, 5, 6)
LEFTS = 7
RIGHTS = 9
BLOCK = 128
WIDE = 512
FULL = 1024
PARTS = 12


def left_of(t):
    return jnp.where(t < 8, t // 2, jnp.where(t < 16, 4, jnp.where(t < 18, 6, 5)))


def right_of(t):
    return jnp.where(t < 8, 0, jnp.where(t < 16, t // 2 - 3, jnp.where(t < 18, 8, t // 2 - 4)))


def add_rows(target, sources, rows):
    def step(i, carry):
        at = pl.ds(pl.multiple_of(i * 16, 16), 16)
        total = sources[0][at].astype(jnp.float32)
        for source in sources[1:]:
            total = total + source[at].astype(jnp.float32)
        target[at] = total.astype(target.dtype)
        return carry

    lax.fori_loop(0, rows // 16, step, 0)


def reduce_kernel(*refs):
    activated, normed_mid, normed_in, attended, grad_mlp = refs[:5]
    sources, weights = refs[5:12], refs[12:16]
    pos_col, pos_row, doc_col, doc_row, router, gain_one, gain_two = refs[16:23]
    out_down, out_up, out_qkv, out_out, out_rows, small_sums = refs[23:29]
    (left, right, part, from_x, from_y, last_x, last_y, from_pair, from_far, sums) = refs[29:39]
    held = refs[39:46]
    slope, packed, middle, routed, taken, grad_branch, score = held
    (tall, broad, grad_norm, grad_middle, grad_attended, partial) = refs[46:52]
    small_sent, small_got = refs[52:54]
    (in_own, in_send, in_recv, rin_own, rin_send, rin_recv) = refs[54:60]
    send, recv, small_send, small_recv, stored, held_in, tall_in, broad_in = refs[60:68]
    full_qkv, full_out, full_up, full_down = weights

    z, f, core, along_x, along_y, across = places()
    pair, far = flip(z, 1), 3 - z
    inner = (z == 1) | (z == 2)
    outer = (z == 0) | (z == 3)
    at_core, at_x, at_y = (z, core), (z, along_x), (z, along_y)
    at_pair, at_far = (pair, f), (far, f)
    greet((at_core, at_x, at_y, at_pair, at_far))

    rows = grad_mlp.shape[0]
    mine = pl.ds(pl.multiple_of((f % 2) * rows, rows), rows)
    half = BLOCK // 2
    top, bottom = pl.ds(0, half), pl.ds(half, half)

    def left_source(i):
        if i < 4:
            return activated, 4 * BLOCK, i * BLOCK
        return (normed_mid, normed_in, attended)[i - 4], BLOCK, 0


    def spread(index):
        return (index, flip(index, 2), flip(index, 4), flip(flip(index, 2), 4))

    def left_copies(i):
        source, stride, offset = left_source(i)
        here, there = [], []
        for slot in range(4):
            target = left.at[i, mine, pl.ds(slot * BLOCK, BLOCK)]
            columns = [
                pl.ds(pl.multiple_of(spread(index)[slot] * stride + offset, BLOCK), BLOCK)
                for index in (f, core)
            ]
            here.append(
                pltpu.make_async_copy(source.at[:, columns[0]], target, in_own.at[i, slot])
            )
            there.append(
                pltpu.make_async_remote_copy(
                    src_ref=source.at[:, columns[1]],
                    dst_ref=target,
                    send_sem=in_send.at[i, slot],
                    recv_sem=in_recv.at[i, slot],
                    device_id=at_core,
                    device_id_type=MESH,
                )
            )
        return here + there

    def right_copies(i):
        target = right.at[i, mine]
        source = grad_mlp if i == 0 else target
        there = pltpu.make_async_remote_copy(
            src_ref=source,
            dst_ref=target,
            send_sem=rin_send.at[i],
            recv_sem=rin_recv.at[i],
            device_id=at_core,
            device_id_type=MESH,
        )
        return [there] if i else [there, pltpu.make_async_copy(source, target, rin_own.at[0])]

    lefts = [left_copies(i) for i in range(LEFTS)]
    rights = [right_copies(i) for i in range(RIGHTS)]
    new_left = {0: 0, 2: 1, 4: 2, 6: 3, 8: 4, 16: 6, 18: 5}
    new_right = {0: 0, 8: 1, 10: 2, 12: 3, 14: 4, 16: 8, 18: 5, 20: 6, 22: 7}
    for t in range(CHUNKS):
        for copy in lefts[new_left[t]] if t in new_left else ():
            copy.start()
        for copy in rights[0] if t == 0 else ():
            copy.start()

    loads = [pltpu.make_async_copy(sources[i], held[i], held_in.at[i]) for i in range(7)]
    for load in loads:
        load.start()

    def tall_copy(source, j, slot):
        return pltpu.make_async_copy(source.at[tile(j, 512)], tall.at[slot], tall_in.at[slot])

    def broad_copy(source, j, slot):
        target = broad.at[slot, :, pl.ds(0, source.shape[1])]
        return pltpu.make_async_copy(source.at[tile(j, 256)], target, broad_in.at[slot])

    def turn_down(t):
        for k in range(2):
            slot = t % 2 * 2 + k
            tall_copy(full_down, 2 * t + k, slot).wait()
            at = pl.ds(k * 512, 512)
            grown = dot(right[0, mine], tall[slot], ((1,), (1,)))
            grown = grown * slope[:, tile(2 * t + k, 512)]
            right[t + 1, mine, at] = grown.astype(jnp.bfloat16)

    def turn_up(t):
        slot = t % 2
        broad_copy(full_up, t, slot).wait()
        total = dot(right[1, mine], broad[slot, :, 0:FULL], ((1,), (1,)))
        for k in range(1, 4):
            total += dot(right[1 + k, mine], broad[slot, :, k * FULL : (k + 1) * FULL], ((1,), (1,)))
        grad_norm[:, tile(t, 256)] = total

    def norm_turn(values, ahead, gain):
        inverse = inverse_size(values)
        scaled = ahead * gain
        mean = jnp.mean(scaled * values, axis=-1, keepdims=True)
        back = inverse * scaled - values * (inverse * inverse * inverse * mean)
        return back, jnp.sum(ahead * values * inverse, axis=0, keepdims=True)

    def turn_middle(i):
        at = tile(i, 64)
        back, gain_part = norm_turn(middle[at], grad_norm[at], gain_two[...])
        grad_middle[at] = back
        lower = pl.ds(pl.multiple_of((f % 2) * rows + i * 64, 64), 64)
        right[8, lower] = (grad_branch[at] + back).astype(jnp.bfloat16)
        partial[2:3] += gain_part
        partial[0:1] += jnp.sum(score[at, 0:1] * routed[at], axis=0, keepdims=True)

    def turn_out():
        for k in range(2):
            tall_copy(full_out, k, k).wait()
            grad_attended[:, k * 512 : (k + 1) * 512] = dot(
                right[8, mine], tall[k], ((1,), (1,))
            ).astype(jnp.bfloat16)

    def turn_heads(i):
        query, keys, values = (packed[:, tile(i + 8 * k, 128)] for k in range(3))
        ahead = grad_attended[:, tile(i, 128)]
        allowed = (doc_col[...] == doc_row[...]) & (pos_row[...] <= pos_col[...])
        low = lane_half(query.shape)
        zero = jnp.zeros_like(query)
        found = []
        for keep in (low, ~low):
            probs = head_probs(jnp.where(keep, query, zero), keys, allowed)
            grad_prob = dot(jnp.where(keep, ahead, zero), values, ((1,), (1,)))
            row_dot = jnp.sum(grad_prob * probs, axis=-1, keepdims=True)
            grad_scores = (probs * (grad_prob - row_dot)).astype(jnp.bfloat16)
            found.append(
                (
                    dot(grad_scores, keys) * 0.125,
                    dot(grad_scores, query, ((0,), (0,))) * 0.125,
                    dot(probs.astype(jnp.bfloat16), ahead, ((0,), (0,))),
                )
            )
        for k in range(3):
            mixed = jnp.where(low, found[0][k], found[1][k]).astype(jnp.bfloat16)
            right[5 + k, mine, tile(i, 128)] = mixed

    def turn_in(t):
        slot = t % 2
        broad_copy(full_qkv, t, slot).wait()
        total = dot(right[5, mine], broad[slot, :, 0:FULL], ((1,), (1,)))
        for k in range(1, 3):
            total += dot(right[5 + k, mine], broad[slot, :, k * FULL : (k + 1) * FULL], ((1,), (1,)))
        grad_norm[:, tile(t, 256)] = total

    def turn_rows(i):
        at = tile(i, 64)
        back, gain_part = norm_turn(routed[at], grad_norm[at], gain_one[...])
        partial[1:2] += gain_part
        total = back + grad_middle[at] + score[at, 0:1] * router[...]
        grad_attended[at] = (taken[at].astype(jnp.float32) + total).astype(jnp.bfloat16)

    def work(t):
        @pl.when(t == 0)
        def _():
            loads[0].wait()

        @pl.when(t < 3)
        def _():
            for k in range(2):
                tall_copy(full_down, 2 * t + 2 + k, (t + 1) % 2 * 2 + k).start()

        @pl.when(t < 4)
        def _():
            turn_down(t)
            for i in range(4):

                @pl.when(t == i)
                def _(i=i):
                    rights[1 + i][0].start()

        @pl.when((t >= 3) & (t < 7))
        def _():
            broad_copy(full_up, t - 3, (t - 3) % 2).start()

        @pl.when((t >= 4) & (t < 8))
        def _():
            turn_up(t - 4)

        @pl.when(t == 7)
        def _():
            for k in range(2):
                tall_copy(full_out, k, k).start()
            for load in loads[1:]:
                load.wait()

        @pl.when(t == 8)
        def _():
            partial[...] = jnp.zeros_like(partial)
            each(4, turn_middle)
            rights[8][0].start()

        @pl.when(t == 9)
        def _():
            turn_out()

        @pl.when((t >= 10) & (t < 18))
        def _():
            turn_heads(t - 10)

        @pl.when(t == 17)
        def _():
            for i in (5, 6, 7):
                rights[i][0].start()

        @pl.when((t >= 17) & (t < 21))
        def _():
            broad_copy(full_qkv, t - 17, (t - 17) % 2).start()

        @pl.when((t >= 18) & (t < 22))
        def _():
            turn_in(t - 18)

        @pl.when(t == 22)
        def _():
            each(4, turn_rows)
            small_sent[0] = partial[...]
            small_copy(0).start()
            pltpu.make_async_copy(grad_attended, out_rows, held_in.at[0]).start()

        @pl.when(t == 28)
        def _():
            pltpu.make_async_copy(grad_attended, out_rows, held_in.at[0]).wait()

    for k in range(2):
        tall_copy(full_down, k, k).start()

    def remote(t, kind, source, target, peer):
        return pltpu.make_async_remote_copy(
            src_ref=source,
            dst_ref=target,
            send_sem=send.at[t, kind],
            recv_sem=recv.at[t, kind],
            device_id=peer,
            device_id_type=MESH,
        )

    def moved(t, kind):
        source, target, peer = (
            lambda: (part.at[t % PARTS, 1, top], from_x.at[t, 0], at_x),
            lambda: (part.at[t % PARTS, 3, top], from_x.at[t, 1], at_x),
            lambda: (part.at[t % PARTS, 2, bottom], from_y.at[t, 0], at_y),
            lambda: (part.at[t % PARTS, 3, bottom], from_y.at[t, 1], at_y),
            lambda: (part.at[t % PARTS, 1, bottom], last_x.at[t], at_x),
            lambda: (part.at[t % PARTS, 2, top], last_y.at[t], at_y),
            lambda: (part.at[t % PARTS, 0], from_pair.at[t], at_pair),
            lambda: (part.at[t % PARTS, 0], from_far.at[t], at_far),
            lambda: (sums.at[t], sums.at[t], at_pair),
        )[kind]()
        return remote(t, kind, source, target, peer)

    def stage_product(t):
        lhs = left[left_of(t)]
        for column in range(0, WIDE, 256):
            block = lax.dot_general(
                lhs,
                right[right_of(t), :, pl.ds(pl.multiple_of((t % 2) * WIDE + column, 256), 256)],
                (((0,), (0,)), ((), ())),
                preferred_element_type=jnp.float32,
            ).astype(jnp.bfloat16)
            for slot in range(4):
                part[t % PARTS, slot, :, column : column + 256] = block[slot * BLOCK : (slot + 1) * BLOCK]
        for kind in (1, 3, 0, 2):
            moved(t, kind).start()

    def stage_turn(t):
        moved(t, 1).wait_recv()
        add_rows(part.at[t % PARTS, 2, top], (part.at[t % PARTS, 2, top], from_x.at[t, 1]), half)
        moved(t, 5).start()
        moved(t, 3).wait_recv()
        add_rows(part.at[t % PARTS, 1, bottom], (part.at[t % PARTS, 1, bottom], from_y.at[t, 1]), half)
        moved(t, 4).start()

    def stage_plane(t):
        moved(t, 0).wait_recv()
        moved(t, 5).wait_recv()
        add_rows(part.at[t % PARTS, 0, top], (part.at[t % PARTS, 0, top], from_x.at[t, 0], last_y.at[t]), half)
        moved(t, 2).wait_recv()
        moved(t, 4).wait_recv()
        add_rows(
            part.at[t % PARTS, 0, bottom], (part.at[t % PARTS, 0, bottom], from_y.at[t, 0], last_x.at[t]), half
        )

        @pl.when(outer)
        def _():
            moved(t, 6).start()

    def stage_pair(t):
        @pl.when(inner)
        def _():
            moved(t, 6).wait_recv()
            add_rows(part.at[t % PARTS, 0], (part.at[t % PARTS, 0], from_pair.at[t]), BLOCK)
            moved(t, 7).start()

    def stage_far(t):
        @pl.when(inner)
        def _():
            moved(t, 7).wait_recv()
            add_rows(sums.at[t], (part.at[t % PARTS, 0], from_far.at[t]), BLOCK)
            moved(t, 8).start()

    def stage_end(t):
        @pl.when(inner)
        def _():
            moved(t, 7).wait_send()
            moved(t, 8).wait_send()

        @pl.when(outer)
        def _():
            moved(t, 6).wait_send()
            moved(t, 8).wait_recv()

        for kind in range(6):
            moved(t, kind).wait_send()

        store(t, True)

    def store(t, begin):
        for low, high, target in (
            (0, 8, lambda i: out_down.at[pl.ds(pl.multiple_of(i // 2 * BLOCK, BLOCK), BLOCK), columns(i % 2)]),
            (8, 16, lambda i: out_up.at[:, columns(i)]),
            (16, 18, lambda i: out_out.at[:, columns(i)]),
            (18, 24, lambda i: out_qkv.at[:, columns(i)]),
        ):

            @pl.when((t >= low) & (t < high))
            def _(low=low, target=target):
                copy = pltpu.make_async_copy(sums.at[t], target(t - low), stored.at[t])
                copy.start() if begin else copy.wait()

    def columns(i):
        return pl.ds(pl.multiple_of(i * WIDE, WIDE), WIDE)

    def stage_stored(t):
        store(t, False)

    peers = (at_core, at_x, at_y, at_pair, at_far)

    def small_copy(j):
        return pltpu.make_async_remote_copy(
            src_ref=small_sent.at[j],
            dst_ref=small_got.at[j],
            send_sem=small_send.at[j],
            recv_sem=small_recv.at[j],
            device_id=peers[j],
            device_id_type=MESH,
        )

    stages = (stage_turn, stage_plane, stage_pair, stage_far, stage_end, stage_stored)

    def tick(t, carry):
        for when, i in new_left.items():

            @pl.when(t == when)
            def _(i=i):
                for copy in lefts[i]:
                    copy.wait()

        for when, i in new_right.items():

            @pl.when(t == when)
            def _(i=i):
                for copy in rights[i]:
                    copy.wait()

        @pl.when(t < CHUNKS)
        def _():
            stage_product(t)

        work(t)
        for lag, stage in zip(LAGS, stages):

            @pl.when((t >= lag) & (t < CHUNKS + lag))
            def _(lag=lag, stage=stage):
                stage(t - lag)

        for j in range(5):

            @pl.when(t == 23 + j)
            def _(j=j):
                small_copy(j).wait()
                total = small_sent[j] + small_got[j]
                if j < 4:
                    small_sent[j + 1] = total
                    small_copy(j + 1).start()
                else:
                    small_sums[...] = total

        return carry

    lax.fori_loop(0, CHUNKS + LAGS[-1], tick, 0)


def run_backward(lefts, grad_mlp, sources, weights, positions, documents, router, gain_one, gain_two):
    rows = grad_mlp.shape[0]
    bf16, f32, dma = jnp.bfloat16, jnp.float32, pltpu.SemaphoreType.DMA
    chunk, half_chunk = (CHUNKS, BLOCK, WIDE), (CHUNKS, BLOCK // 2, WIDE)
    held = [
        ((LEFTS, 2 * rows, 4 * BLOCK), bf16),
        ((RIGHTS, 2 * rows, FULL), bf16),
        ((PARTS, 4, BLOCK, WIDE), bf16),
        ((CHUNKS, 2, BLOCK // 2, WIDE), bf16),
        ((CHUNKS, 2, BLOCK // 2, WIDE), bf16),
        (half_chunk, bf16),
        (half_chunk, bf16),
        (chunk, bf16),
        (chunk, bf16),
        (chunk, bf16),
    ]
    held += [(source.shape, source.dtype) for source in sources]
    held += [
        ((4, 512, FULL), bf16),
        ((2, 256, 4 * FULL), bf16),
        ((rows, FULL), f32),
        ((rows, FULL), f32),
        ((rows, FULL), bf16),
        ((8, FULL), f32),
        ((5, 8, FULL), f32),
        ((5, 8, FULL), f32),
    ]
    counts = [(LEFTS, 4)] * 3 + [(RIGHTS,)] * 3 + [(CHUNKS, 9)] * 2 + [(5,)] * 2
    counts += [(CHUNKS,), (7,), (4,), (2,)]
    shapes = [(4 * BLOCK, FULL), (BLOCK, 4 * FULL), (BLOCK, 3 * FULL), (BLOCK, FULL), (rows, FULL)]
    return pl.pallas_call(
        reduce_kernel,
        out_shape=[jax.ShapeDtypeStruct(shape, bf16) for shape in shapes]
        + [jax.ShapeDtypeStruct((8, FULL), f32)],
        in_specs=[pl.BlockSpec(memory_space=ANY)] * 16
        + [pl.BlockSpec(memory_space=pltpu.VMEM)] * 7,
        out_specs=[pl.BlockSpec(memory_space=ANY)] * 5 + [pl.BlockSpec(memory_space=pltpu.VMEM)],
        scratch_shapes=[pltpu.VMEM(*each_one) for each_one in held] + [dma(count) for count in counts],
        compiler_params=pltpu.CompilerParams(
            collective_id=2, has_side_effects=True, vmem_limit_bytes=62 * 1024 * 1024
        ),
        name="backward_and_reduce",
    )(
        *lefts,
        grad_mlp,
        *sources,
        *weights,
        positions[:, None],
        positions[None],
        documents[:, None],
        documents[None],
        router[None],
        gain_one[None],
        gain_two[None],
    )


def put_rows(tokens, rows, positions):
    hit = lax.broadcasted_iota(jnp.int32, (tokens.shape[0], positions.shape[0]), 0) == positions[None]
    moved = jnp.dot(hit.astype(jnp.bfloat16), rows, preferred_element_type=jnp.float32)
    return jnp.where(jnp.any(hit, axis=1, keepdims=True), moved.astype(jnp.bfloat16), tokens)


def per_device(
    hidden, cotangent, route_pos, route_doc, w_qkv, w_out, w_up, w_down, router, gain_one, gain_two
):
    positions = route_pos[0]
    documents = route_doc[0]
    (
        full_qkv,
        full_out,
        full_up,
        full_down,
        routed,
        taken,
        normed_in,
        packed,
        attended,
        middle,
        normed_mid,
        activated,
        slope,
        grad_mlp,
        grad_branch,
        rows_out,
        score,
    ) = run_forward(
        (w_qkv, w_out, w_up, w_down),
        8,
        hidden,
        cotangent,
        positions,
        documents,
        router,
        gain_one,
        gain_two,
    )
    output = put_rows(hidden, rows_out, positions)
    *sums, grad_rows, small_sums = run_backward(
        (activated, normed_mid, normed_in, attended),
        grad_mlp,
        (slope, packed, middle, routed, taken, grad_branch, score),
        (full_qkv, full_out, full_up, full_down),
        positions,
        documents,
        router,
        gain_one,
        gain_two,
    )
    grad_hidden = put_rows(cotangent, grad_rows, positions)
    sum_down, sum_up, sum_qkv, sum_out = (total.astype(jnp.float32) for total in sums)
    return (
        output,
        grad_hidden,
        sum_qkv,
        sum_out,
        sum_up,
        sum_down,
        small_sums[0],
        small_sums[1],
        small_sums[2],
    )


def solution(mesh):
    paired = dict(mesh.shape) == {"dp": 4, "fsdp": 8}
    tokens, weights = P(("dp", "fsdp"), None), P("fsdp", None)
    return jax.shard_map(
        per_device if paired else general_device,
        mesh=mesh,
        in_specs=(tokens,) * 4 + (weights,) * 4 + (P(),) * 3,
        out_specs=(tokens,) * 2 + (weights,) * 4 + (P(),) * 3,
        check_vma=False,
    )
```

```python
import functools

import jax
import jax.numpy as jnp
from jax import lax
from jax.experimental import pallas as pl
from jax.experimental.pallas import tpu as pltpu
from jax.sharding import PartitionSpec as P

D = 1024
HEADS = 16
HEAD = 64


EPS = 1e-06


def rms_scale(values, gain_vec):
    return values * lax.rsqrt(jnp.mean(values * values, axis=-1, keepdims=True) + EPS) * gain_vec


def forward(tokens, positions, documents, weights, router, gain_one, gain_two):
    full_qkv, full_out, full_up, full_down = weights
    routed = tokens[positions].astype(jnp.float32)
    row_count = routed.shape[0]
    router_out = jnp.dot(routed, router, precision=lax.Precision.HIGHEST)
    normed_in = rms_scale(routed, gain_one).astype(jnp.bfloat16)
    packed = jnp.dot(normed_in, full_qkv, preferred_element_type=jnp.float32).astype(jnp.bfloat16)
    heads = packed.reshape(row_count, 3, HEADS, HEAD)
    allowed = (documents[:, None] == documents[None, :]) & (
        positions[None, :] <= positions[:, None]
    )
    scores = (
        jnp.einsum("qhd,khd->hqk", heads[:, 0], heads[:, 1], preferred_element_type=jnp.float32)
        * 0.125
    )
    scores = jnp.where(allowed[None], scores, -1000000000.0)
    row_max = jnp.max(scores, axis=-1, keepdims=True)
    log_total = row_max + jnp.log(jnp.sum(jnp.exp(scores - row_max), axis=-1, keepdims=True))
    prob_rows = jnp.exp(scores - log_total)
    prob_low = prob_rows.astype(jnp.bfloat16)
    attended = jnp.einsum("hqk,khd->qhd", prob_low, heads[:, 2], preferred_element_type=jnp.float32)
    attended = attended.reshape(row_count, D).astype(jnp.bfloat16)
    attn_out = jnp.dot(attended, full_out, preferred_element_type=jnp.float32)
    middle = routed + attn_out
    normed_mid = rms_scale(middle, gain_two).astype(jnp.bfloat16)
    up_in = jnp.dot(normed_mid, full_up, preferred_element_type=jnp.float32)
    activated = jax.nn.gelu(up_in).astype(jnp.bfloat16)
    mlp_out = jnp.dot(activated, full_down, preferred_element_type=jnp.float32)
    return (
        routed,
        router_out,
        normed_in,
        heads,
        prob_rows,
        prob_low,
        attended,
        attn_out,
        middle,
        normed_mid,
        up_in,
        activated,
        mlp_out,
    )


def general_device(
    hidden, cotangent, route_pos, route_doc, w_qkv, w_out, w_up, w_down, router, gain_one, gain_two
):
    positions = route_pos[0]
    documents = route_doc[0]
    live_mask = (documents < 2).astype(jnp.float32)[:, None]
    gathered = (
        lax.all_gather(w_qkv, "fsdp", axis=0, tiled=True),
        lax.all_gather(w_out, "fsdp", axis=0, tiled=True),
        lax.all_gather(w_up, "fsdp", axis=0, tiled=True),
        lax.all_gather(w_down, "fsdp", axis=0, tiled=True),
    )
    state = forward(hidden, positions, documents, gathered, router, gain_one, gain_two)
    attn_first = state[7]
    mlp_first = state[12]
    added = live_mask * state[1][:, None] * (attn_first + mlp_first)
    output = hidden.astype(jnp.float32).at[positions].add(added).astype(jnp.bfloat16)
    weights = (
        lax.all_gather(w_qkv, "fsdp", axis=0, tiled=True),
        lax.all_gather(w_out, "fsdp", axis=0, tiled=True),
        lax.all_gather(w_up, "fsdp", axis=0, tiled=True),
        lax.all_gather(w_down, "fsdp", axis=0, tiled=True),
    )
    state = forward(hidden, positions, documents, weights, router, gain_one, gain_two)
    full_qkv, full_out, full_up, full_down = weights
    (
        routed,
        router_out,
        normed_in,
        heads,
        prob_rows,
        prob_low,
        attended,
        attn_out,
        middle,
        normed_mid,
        up_in,
        activated,
        mlp_out,
    ) = state
    row_count = routed.shape[0]
    branch_out = attn_out + mlp_out
    grad_add = live_mask * cotangent[positions].astype(jnp.float32)
    grad_branch = grad_add * router_out[:, None]
    grad_score = jnp.sum(grad_add * branch_out, axis=-1)
    grad_mlp = grad_branch.astype(jnp.bfloat16)
    grad_down = jnp.dot(activated.T, grad_mlp, preferred_element_type=jnp.float32)
    grad_act = jnp.dot(grad_mlp, full_down.T, preferred_element_type=jnp.float32)
    _, gelu_pull = jax.vjp(jax.nn.gelu, up_in)
    grad_up_in = gelu_pull(grad_act)[0].astype(jnp.bfloat16)
    grad_up = jnp.dot(normed_mid.T, grad_up_in, preferred_element_type=jnp.float32)
    grad_norm_mid = jnp.dot(grad_up_in, full_up.T, preferred_element_type=jnp.float32)
    _, second_pull = jax.vjp(rms_scale, middle, gain_two)
    grad_middle, grad_gain_two = second_pull(grad_norm_mid)
    grad_attn = (grad_branch + grad_middle).astype(jnp.bfloat16)
    grad_out = jnp.dot(attended.T, grad_attn, preferred_element_type=jnp.float32)
    grad_attended = jnp.dot(grad_attn, full_out.T, preferred_element_type=jnp.float32).astype(
        jnp.bfloat16
    )
    grad_attended = grad_attended.reshape(row_count, HEADS, HEAD)
    grad_prob = jnp.einsum(
        "qhd,khd->hqk", grad_attended, heads[:, 2], preferred_element_type=jnp.float32
    )
    grad_value = jnp.einsum(
        "hqk,qhd->khd", prob_low, grad_attended, preferred_element_type=jnp.float32
    )
    row_dot = jnp.sum(grad_prob * prob_rows, axis=-1, keepdims=True)
    grad_scores = (prob_rows * (grad_prob - row_dot)).astype(jnp.bfloat16)
    grad_query = (
        jnp.einsum("hqk,khd->qhd", grad_scores, heads[:, 1], preferred_element_type=jnp.float32)
        * 0.125
    )
    grad_key = (
        jnp.einsum("hqk,qhd->khd", grad_scores, heads[:, 0], preferred_element_type=jnp.float32)
        * 0.125
    )
    grad_packed = jnp.stack([grad_query, grad_key, grad_value], axis=1).reshape(row_count, 3 * D)
    grad_packed = grad_packed.astype(jnp.bfloat16)
    grad_qkv = jnp.dot(normed_in.T, grad_packed, preferred_element_type=jnp.float32)
    grad_norm_in = jnp.dot(grad_packed, full_qkv.T, preferred_element_type=jnp.float32)
    _, first_pull = jax.vjp(rms_scale, routed, gain_one)
    grad_routed, grad_gain_one = first_pull(grad_norm_in)
    grad_routed = grad_routed + grad_middle + grad_score[:, None] * router[None, :]
    grad_router = jnp.dot(grad_score, routed, precision=lax.Precision.HIGHEST)
    grad_hidden = cotangent.astype(jnp.float32).at[positions].add(grad_routed).astype(jnp.bfloat16)
    shard_sums = (
        lax.psum_scatter(grad_qkv.astype(jnp.bfloat16), "fsdp", scatter_dimension=0, tiled=True),
        lax.psum_scatter(grad_out.astype(jnp.bfloat16), "fsdp", scatter_dimension=0, tiled=True),
        lax.psum_scatter(grad_up.astype(jnp.bfloat16), "fsdp", scatter_dimension=0, tiled=True),
        lax.psum_scatter(grad_down.astype(jnp.bfloat16), "fsdp", scatter_dimension=0, tiled=True),
    )
    final_sums = lax.psum((shard_sums[0], shard_sums[1], shard_sums[2], shard_sums[3]), "dp")
    small_sums = lax.psum((grad_router, grad_gain_one, grad_gain_two), ("dp", "fsdp"))
    return (
        output,
        grad_hidden,
        final_sums[0].astype(jnp.float32),
        final_sums[1].astype(jnp.float32),
        final_sums[2].astype(jnp.float32),
        final_sums[3].astype(jnp.float32),
        small_sums[0],
        small_sums[1],
        small_sums[2],
    )


MESH = pl.DeviceIdType.MESH
ANY = pl.ANY


def flip(index, stride):
    return index + stride - 2 * stride * ((index // stride) % 2)


def places():
    z = lax.axis_index("dp")
    f = lax.axis_index("fsdp")
    return z, f, flip(f, 1), flip(f, 2), flip(f, 4), flip(flip(f, 2), 4)


def greet(peers):
    barrier = pltpu.get_barrier_semaphore()
    for peer in peers:
        pl.semaphore_signal(barrier, inc=1, device_id=peer, device_id_type=MESH)
    pl.semaphore_wait(barrier, len(peers))


GATHER_KINDS = 13


ROOT = 0.7978845608028654
CUBE = 0.044715
EPSILON = 1e-06


def tile(i, size):
    return pl.ds(pl.multiple_of(i * size, size), size)


def each(count, fn):
    def step(i, carry):
        fn(i)
        return carry

    lax.fori_loop(0, count, step, 0)


def dot(left, right, dims=((1,), (0,))):
    return lax.dot_general(left, right, (dims, ((), ())), preferred_element_type=jnp.float32)


def inverse_size(values):
    return lax.rsqrt(jnp.mean(values * values, axis=-1, keepdims=True) + EPSILON)


def upright(row):
    return jnp.broadcast_to(row.astype(jnp.float32), (128, row.shape[1])).T.astype(jnp.int32)


def lane_half(shape):
    return lax.broadcasted_iota(jnp.int32, shape, 1) < HEAD


def head_probs(query, keys, allowed):
    scores = jnp.where(allowed, dot(query, keys, ((1,), (1,))) * 0.125, -1000000000.0)
    raised = jnp.exp(scores - jnp.max(scores, axis=-1, keepdims=True))
    return raised / jnp.sum(raised, axis=-1, keepdims=True)


def forward_kernel(*refs):
    shards = refs[0:4]
    hidden, cotangent, pos_row, doc_row, router, gain_one, gain_two = refs[4:11]
    outs = refs[11:28]
    fulls = refs[28:31] + (outs[3],)
    (tokens, cotokens, hit, routed, taken, normed_in, packed, attended, attn_out, middle) = refs[31:41]
    (normed_mid, slope, activated, grad_mlp, grad_branch, gate) = refs[41:47]
    kept_down, pos_col, doc_col = refs[47:50]
    own_in, token_in, out_sem, send, recv = refs[50:55]
    z, f, core, along_x, along_y, across = places()
    pair = flip(z, 1)
    at_core, at_x, at_y, at_z = (z, core), (z, along_x), (z, along_y), (pair, f)
    greet((at_core, at_x, at_y, at_z))
    count = routed.shape[0]
    part = count // 4

    def rows_of(w, origin, start, size):
        rows = shards[w].shape[0]
        return pl.ds(pl.multiple_of(origin * rows + start, 16), size)

    def copy(w, kind, source, origin, start, size, peer):
        return pltpu.make_async_remote_copy(
            src_ref=source,
            dst_ref=fulls[w].at[rows_of(w, origin, start, size)],
            send_sem=send.at[w, kind],
            recv_sem=recv.at[w, kind],
            device_id=peer,
            device_id_type=MESH,
        )

    def own(w, kind, start, size, peer):
        source = shards[w].at[pl.ds(pl.multiple_of(start, 16), size)]
        return copy(w, kind, source, f, start, size, peer)

    def passed(w, kind, origin, start, size, peer):
        return copy(w, kind, fulls[w].at[rows_of(w, origin, start, size)], origin, start, size, peer)

    plan = []
    for w in range(4):
        rows = shards[w].shape[0]
        half = rows // 2
        even, odd = (z % 2) * half, (1 - z % 2) * half
        plan.append(
            [
                own(w, 0, even, half, at_x),
                own(w, 1, odd, half, at_y),
                own(w, 2, 0, rows, at_core),
                passed(w, 3, along_y, odd, half, at_x),
                passed(w, 4, along_x, even, half, at_y),
                passed(w, 5, along_x, even, half, at_z),
                passed(w, 6, along_y, odd, half, at_z),
                passed(w, 7, along_x, even, half, at_core),
                passed(w, 8, along_y, odd, half, at_core),
                passed(w, 9, across, odd, half, at_core),
                passed(w, 10, across, even, half, at_core),
                passed(w, 11, along_x, odd, half, at_core),
                passed(w, 12, along_y, even, half, at_core),
            ]
        )

    def first(w):
        for kind in (0, 1, 2):
            plan[w][kind].start()

    def second(w):
        plan[w][0].wait_recv()
        for kind in (5, 4, 7):
            plan[w][kind].start()
        plan[w][1].wait_recv()
        for kind in (6, 3, 8):
            plan[w][kind].start()

    def third(w):
        for kind, onward in ((3, 9), (4, 10), (5, 11), (6, 12)):
            plan[w][kind].wait_recv()
            plan[w][onward].start()

    def finish(w):
        if w < 3:
            loads[w].wait()
        else:
            store_down.wait()
        for kind in (2,) + tuple(range(7, GATHER_KINDS)):
            plan[w][kind].wait_recv()
        if w < 3:
            put(w, fulls[w])

    def put(i, source):
        pltpu.make_async_copy(source, outs[i], out_sem.at[i]).start()

    def settle(i, source):
        pltpu.make_async_copy(source, outs[i], out_sem.at[i]).wait()

    own_places = [fulls[w].at[rows_of(w, f, 0, shards[w].shape[0])] for w in range(4)]
    loads = [
        pltpu.make_async_copy(shards[w], kept_down if w == 3 else own_places[w], own_in.at[w])
        for w in range(4)
    ]
    store_down = pltpu.make_async_copy(kept_down, own_places[3], own_in.at[4])
    token_loads = [
        pltpu.make_async_copy(hidden, tokens, token_in.at[0]),
        pltpu.make_async_copy(cotangent, cotokens, token_in.at[1]),
    ]
    first(1)
    first(0)
    for load in token_loads + loads:
        load.start()
    pos_col[...] = upright(pos_row[...])
    doc_col[...] = upright(doc_row[...])

    def mark(i):
        slots = lax.broadcasted_iota(jnp.int32, (part, hit.shape[1]), 1)
        hit[tile(i, part)] = (slots == pos_col[tile(i, part), 0:1]).astype(jnp.bfloat16)

    each(4, mark)

    def take(source, target):
        def columns(n):
            target[:, tile(n, 256)] = dot(hit[...], source[:, tile(n, 256)]).astype(target.dtype)

        each(D // 256, columns)

    token_loads[0].wait()
    take(tokens, routed)
    token_loads[1].wait()
    take(cotokens, taken)

    def open_rows(i):
        at = tile(i, part)
        rows = routed[at]
        normed_in[at] = (rows * inverse_size(rows) * gain_one[...]).astype(jnp.bfloat16)
        router_out = jnp.sum(rows * router[...], axis=-1, keepdims=True)
        gate_rows = jnp.where(doc_col[at, 0:1] < 2, router_out, 0.0)
        gate[at] = jnp.broadcast_to(gate_rows, (part, 128))
        grad_rows = taken[at].astype(jnp.float32) * gate_rows
        grad_branch[at] = grad_rows
        grad_mlp[at] = grad_rows.astype(jnp.bfloat16)

    each(4, open_rows)
    for i, source in ((4, routed), (5, taken), (6, normed_in), (13, grad_mlp), (14, grad_branch)):
        put(i, source)
    put(16, gate)
    loads[3].wait()
    store_down.start()
    second(1)
    first(2)
    second(0)
    first(3)
    second(2)
    third(1)
    finish(1)
    third(0)
    finish(0)

    def pack(n):
        packed[:, tile(n, 512)] = dot(normed_in[...], fulls[0][:, tile(n, 512)]).astype(jnp.bfloat16)

    each(6, pack)
    put(7, packed)

    def attend(i):
        query, keys, values = (packed[:, tile(i + 8 * k, 128)] for k in range(3))
        allowed = (doc_col[:, 0:1] == doc_row[...]) & (pos_row[...] <= pos_col[:, 0:1])
        low = lane_half(query.shape)
        zero = jnp.zeros_like(query)
        mixed = [
            dot(head_probs(jnp.where(keep, query, zero), keys, allowed).astype(jnp.bfloat16), values)
            for keep in (low, ~low)
        ]
        attended[:, tile(i, 128)] = jnp.where(low, mixed[0], mixed[1]).astype(jnp.bfloat16)

    each(HEADS // 4, attend)
    second(3)
    each(HEADS // 4, lambda i: attend(i + HEADS // 4))
    put(8, attended)

    def project(n):
        attn_out[:, tile(n, 256)] = dot(attended[...], fulls[1][:, tile(n, 256)])

    each(4, project)

    def middle_rows(i):
        at = tile(i, part)
        rows = routed[at] + attn_out[at]
        middle[at] = rows
        normed_mid[at] = (rows * inverse_size(rows) * gain_two[...]).astype(jnp.bfloat16)

    each(4, middle_rows)
    put(9, middle)
    put(15, attn_out)
    put(10, normed_mid)
    third(2)
    finish(2)

    def raise_up(n):
        at = tile(n, 256)
        up = dot(normed_mid[...], fulls[2][:, at])
        square = up * up
        bend = jnp.tanh(ROOT * (up + CUBE * (square * up)))
        ahead = 0.5 * (1.0 + bend)
        activated[:, at] = (up * ahead).astype(jnp.bfloat16)
        slope[:, at] = ahead + 0.5 * up * (1.0 - bend * bend) * (ROOT * (1.0 + 3.0 * CUBE * square))

    each(16, raise_up)
    put(11, activated)
    put(12, slope)
    third(3)
    finish(3)

    kept = (routed, taken, normed_in, packed, attended, middle, normed_mid, activated, slope)
    for i, source in enumerate(fulls + kept + (grad_mlp, grad_branch, attn_out, gate)):
        if i != 3:
            settle(i, source)
    for w in range(4):
        for kind in range(GATHER_KINDS):
            plan[w][kind].wait_send()


def run_forward(weights, parts, hidden, cotangent, positions, documents, router, gain_one, gain_two):
    bf16, f32, dma = jnp.bfloat16, jnp.float32, pltpu.SemaphoreType.DMA
    count, wide = positions.shape[0], weights[2].shape[1]
    full = [((w.shape[0] * parts, w.shape[1]), w.dtype) for w in weights]
    row, head_row, wide_row = (count, D), (count, 3 * D), (count, wide)
    kept = [(row, f32), (row, bf16), (row, bf16), (head_row, bf16), (row, bf16), (row, f32)]
    kept += [(row, bf16), (wide_row, bf16), (wide_row, f32), (row, bf16), (row, f32), (row, f32)]
    kept += [((count, 128), f32)]
    held = [(hidden.shape, bf16)] * 2 + [((count, hidden.shape[0]), bf16), (row, f32), (row, bf16)]
    held += [(row, bf16), (head_row, bf16), (row, bf16), (row, f32), (row, f32), (row, bf16)]
    held += [(wide_row, f32), (wide_row, bf16), (row, bf16), (row, f32)]
    held += [((count, 128), f32), (weights[3].shape, bf16)] + [((count, 128), jnp.int32)] * 2
    return pl.pallas_call(
        forward_kernel,
        out_shape=[jax.ShapeDtypeStruct(*each_one) for each_one in full + kept],
        in_specs=[pl.BlockSpec(memory_space=ANY)] * 6
        + [pl.BlockSpec(memory_space=pltpu.VMEM)] * 5,
        out_specs=[pl.BlockSpec(memory_space=ANY)] * 17,
        scratch_shapes=[pltpu.VMEM(*each_one) for each_one in full[:3] + held]
        + [dma((5,)), dma((2,)), dma((17,)), dma((4, GATHER_KINDS)), dma((4, GATHER_KINDS))],
        compiler_params=pltpu.CompilerParams(
            collective_id=1, has_side_effects=True, vmem_limit_bytes=60 * 1024 * 1024
        ),
        name="gather_and_forward",
    )(
        *weights,
        hidden,
        cotangent,
        positions[None],
        documents[None],
        router[None],
        gain_one[None],
        gain_two[None],
    )


CHUNKS = 24
LAGS = (1, 2, 3, 4, 5, 6)
LEFTS = 7
RIGHTS = 9
BLOCK = 128
WIDE = 512
FULL = 1024
PARTS = 12


def left_of(t):
    return jnp.where(t < 8, t // 2, jnp.where(t < 16, 4, jnp.where(t < 18, 6, 5)))


def right_of(t):
    return jnp.where(t < 8, 0, jnp.where(t < 16, t // 2 - 3, jnp.where(t < 18, 8, t // 2 - 4)))


def add_rows(target, sources, rows):
    def step(i, carry):
        at = pl.ds(pl.multiple_of(i * 16, 16), 16)
        total = sources[0][at].astype(jnp.float32)
        for source in sources[1:]:
            total = total + source[at].astype(jnp.float32)
        target[at] = total.astype(target.dtype)
        return carry

    lax.fori_loop(0, rows // 16, step, 0)


def reduce_kernel(*refs):
    activated, normed_mid, normed_in, attended, grad_mlp = refs[:5]
    sources, weights = refs[5:13] + refs[0:1], refs[13:17]
    pos_row, doc_row, router, gain_one, gain_two = refs[17:22]
    out_down, out_up, out_qkv, out_out, out_first, out_rows, small_sums = refs[22:29]
    (left, right, part, from_x, from_y, last_x, last_y, from_pair, from_far, sums) = refs[29:39]
    held = refs[39:48]
    slope, branch, packed, middle, routed, taken, grad_branch, gate, wide = held
    (tall, broad, grad_norm, grad_middle, grad_attended, partial) = refs[48:54]
    small_sent, small_got, score, pos_col, doc_col = refs[54:59]
    (in_own, in_send, in_recv, rin_own, rin_send, rin_recv) = refs[59:65]
    send, recv, small_send, small_recv, stored, held_in, tall_in, broad_in = refs[65:73]
    full_qkv, full_out, full_up, full_down = weights

    z, f, core, along_x, along_y, across = places()
    pair, far = flip(z, 1), 3 - z
    inner = (z == 1) | (z == 2)
    outer = (z == 0) | (z == 3)
    at_core, at_x, at_y = (z, core), (z, along_x), (z, along_y)
    at_pair, at_far = (pair, f), (far, f)
    greet((at_core, at_x, at_y, at_pair, at_far))

    rows = grad_mlp.shape[0]
    mine = pl.ds(pl.multiple_of((f % 2) * rows, rows), rows)
    half = BLOCK // 2
    top, bottom = pl.ds(0, half), pl.ds(half, half)

    def left_source(i):
        if i < 4:
            return activated, 4 * BLOCK, i * BLOCK
        return (normed_mid, normed_in, attended)[i - 4], BLOCK, 0


    def spread(index):
        return (index, flip(index, 2), flip(index, 4), flip(flip(index, 2), 4))

    def left_copies(i):
        source, stride, offset = left_source(i)
        here, there = [], []
        for slot in range(4):
            target = left.at[i, mine, pl.ds(slot * BLOCK, BLOCK)]
            columns = [
                pl.ds(pl.multiple_of(spread(index)[slot] * stride + offset, BLOCK), BLOCK)
                for index in (f, core)
            ]
            here.append(
                pltpu.make_async_copy(source.at[:, columns[0]], target, in_own.at[i, slot])
            )
            there.append(
                pltpu.make_async_remote_copy(
                    src_ref=source.at[:, columns[1]],
                    dst_ref=target,
                    send_sem=in_send.at[i, slot],
                    recv_sem=in_recv.at[i, slot],
                    device_id=at_core,
                    device_id_type=MESH,
                )
            )
        return here + there

    def right_copies(i):
        target = right.at[i, mine]
        source = grad_mlp if i == 0 else target
        there = pltpu.make_async_remote_copy(
            src_ref=source,
            dst_ref=target,
            send_sem=rin_send.at[i],
            recv_sem=rin_recv.at[i],
            device_id=at_core,
            device_id_type=MESH,
        )
        return [there] if i else [there, pltpu.make_async_copy(source, target, rin_own.at[0])]

    lefts = [left_copies(i) for i in range(LEFTS)]
    rights = [right_copies(i) for i in range(RIGHTS)]
    new_left = {0: 0, 2: 1, 4: 2, 6: 3, 8: 4, 16: 6, 18: 5}
    new_right = {0: 0, 8: 1, 10: 2, 12: 3, 14: 4, 16: 8, 18: 5, 20: 6, 22: 7}
    for t in range(CHUNKS):
        for copy in lefts[new_left[t]] if t in new_left else ():
            copy.start()
        for copy in rights[0] if t == 0 else ():
            copy.start()

    loads = [pltpu.make_async_copy(sources[i], held[i], held_in.at[i]) for i in range(9)]
    for i in (0, 8, 1, 2, 3, 4, 5, 6, 7):
        loads[i].start()
    pos_col[...] = upright(pos_row[...])
    doc_col[...] = upright(doc_row[...])

    def tall_copy(source, j, slot):
        return pltpu.make_async_copy(source.at[tile(j, 512)], tall.at[slot], tall_in.at[slot])

    def broad_copy(source, j, slot):
        target = broad.at[slot, :, pl.ds(0, source.shape[1])]
        return pltpu.make_async_copy(source.at[tile(j, 256)], target, broad_in.at[slot])

    def turn_down(t):
        for k in range(2):
            slot = t % 2 * 2 + k
            tall_copy(full_down, 2 * t + k, slot).wait()
            at = pl.ds(k * 512, 512)
            grown = dot(right[0, mine], tall[slot], ((1,), (1,)))
            grown = grown * slope[:, tile(2 * t + k, 512)]
            right[t + 1, mine, at] = grown.astype(jnp.bfloat16)
            branch[...] += dot(wide[:, tile(2 * t + k, 512)], tall[slot])

    def turn_up(t):
        slot = t % 2
        broad_copy(full_up, t, slot).wait()
        total = dot(right[1, mine], broad[slot, :, 0:FULL], ((1,), (1,)))
        for k in range(1, 4):
            total += dot(right[1 + k, mine], broad[slot, :, k * FULL : (k + 1) * FULL], ((1,), (1,)))
        grad_norm[:, tile(t, 256)] = total

    def norm_turn(values, ahead, gain):
        inverse = inverse_size(values)
        scaled = ahead * gain
        mean = jnp.mean(scaled * values, axis=-1, keepdims=True)
        back = inverse * scaled - values * (inverse * inverse * inverse * mean)
        return back, jnp.sum(ahead * values * inverse, axis=0, keepdims=True)

    def turn_middle(i):
        at = tile(i, 64)
        back, gain_part = norm_turn(middle[at], grad_norm[at], gain_two[...])
        grad_middle[at] = back
        lower = pl.ds(pl.multiple_of((f % 2) * rows + i * 64, 64), 64)
        right[8, lower] = (grad_branch[at] + back).astype(jnp.bfloat16)
        partial[2:3] += gain_part
        added = branch[at]
        rows_at = routed[at]
        grad_attended[at] = (rows_at + gate[at, 0:1] * added).astype(jnp.bfloat16)
        grad_add = jnp.where(doc_col[at, 0:1] < 2, taken[at].astype(jnp.float32), 0.0)
        grad_score = jnp.sum(grad_add * added, axis=-1, keepdims=True)
        score[at] = jnp.broadcast_to(grad_score, (64, 128))
        partial[0:1] += jnp.sum(grad_score * rows_at, axis=0, keepdims=True)

    def turn_out():
        for k in range(2):
            tall_copy(full_out, k, k).wait()
            grad_attended[:, k * 512 : (k + 1) * 512] = dot(
                right[8, mine], tall[k], ((1,), (1,))
            ).astype(jnp.bfloat16)

    def turn_heads(i):
        query, keys, values = (packed[:, tile(i + 8 * k, 128)] for k in range(3))
        ahead = grad_attended[:, tile(i, 128)]
        allowed = (doc_col[:, 0:1] == doc_row[...]) & (pos_row[...] <= pos_col[:, 0:1])
        low = lane_half(query.shape)
        zero = jnp.zeros_like(query)
        found = []
        for keep in (low, ~low):
            probs = head_probs(jnp.where(keep, query, zero), keys, allowed)
            grad_prob = dot(jnp.where(keep, ahead, zero), values, ((1,), (1,)))
            row_dot = jnp.sum(grad_prob * probs, axis=-1, keepdims=True)
            grad_scores = (probs * (grad_prob - row_dot)).astype(jnp.bfloat16)
            found.append(
                (
                    dot(grad_scores, keys) * 0.125,
                    dot(grad_scores, query, ((0,), (0,))) * 0.125,
                    dot(probs.astype(jnp.bfloat16), ahead, ((0,), (0,))),
                )
            )
        for k in range(3):
            mixed = jnp.where(low, found[0][k], found[1][k]).astype(jnp.bfloat16)
            right[5 + k, mine, tile(i, 128)] = mixed

    def turn_in(t):
        slot = t % 2
        broad_copy(full_qkv, t, slot).wait()
        total = dot(right[5, mine], broad[slot, :, 0:FULL], ((1,), (1,)))
        for k in range(1, 3):
            total += dot(right[5 + k, mine], broad[slot, :, k * FULL : (k + 1) * FULL], ((1,), (1,)))
        grad_norm[:, tile(t, 256)] = total

    def turn_rows(i):
        at = tile(i, 64)
        back, gain_part = norm_turn(routed[at], grad_norm[at], gain_one[...])
        partial[1:2] += gain_part
        total = back + grad_middle[at] + score[at, 0:1] * router[...]
        grad_attended[at] = (taken[at].astype(jnp.float32) + total).astype(jnp.bfloat16)

    def work(t):
        @pl.when(t == 0)
        def _():
            for i in (0, 8, 1):
                loads[i].wait()

        @pl.when(t < 3)
        def _():
            for k in range(2):
                tall_copy(full_down, 2 * t + 2 + k, (t + 1) % 2 * 2 + k).start()

        @pl.when(t < 4)
        def _():
            turn_down(t)
            for i in range(4):

                @pl.when(t == i)
                def _(i=i):
                    rights[1 + i][0].start()

        @pl.when((t >= 3) & (t < 7))
        def _():
            broad_copy(full_up, t - 3, (t - 3) % 2).start()

        @pl.when((t >= 4) & (t < 8))
        def _():
            turn_up(t - 4)

        @pl.when(t == 7)
        def _():
            for k in range(2):
                tall_copy(full_out, k, k).start()
            for load in loads[2:8]:
                load.wait()

        @pl.when(t == 8)
        def _():
            partial[...] = jnp.zeros_like(partial)
            each(4, turn_middle)
            rights[8][0].start()
            pltpu.make_async_copy(grad_attended, out_first, held_in.at[1]).start()

        @pl.when(t == 9)
        def _():
            pltpu.make_async_copy(grad_attended, out_first, held_in.at[1]).wait()
            turn_out()

        @pl.when((t >= 10) & (t < 18))
        def _():
            turn_heads(t - 10)

        @pl.when(t == 17)
        def _():
            for i in (5, 6, 7):
                rights[i][0].start()

        @pl.when((t >= 17) & (t < 21))
        def _():
            broad_copy(full_qkv, t - 17, (t - 17) % 2).start()

        @pl.when((t >= 18) & (t < 22))
        def _():
            turn_in(t - 18)

        @pl.when(t == 22)
        def _():
            each(4, turn_rows)
            small_sent[0] = partial[...]
            small_copy(0).start()
            pltpu.make_async_copy(grad_attended, out_rows, held_in.at[0]).start()

        @pl.when(t == 28)
        def _():
            pltpu.make_async_copy(grad_attended, out_rows, held_in.at[0]).wait()

    for k in range(2):
        tall_copy(full_down, k, k).start()

    def remote(t, kind, source, target, peer):
        return pltpu.make_async_remote_copy(
            src_ref=source,
            dst_ref=target,
            send_sem=send.at[t, kind],
            recv_sem=recv.at[t, kind],
            device_id=peer,
            device_id_type=MESH,
        )

    def moved(t, kind):
        source, target, peer = (
            lambda: (part.at[t % PARTS, 1, top], from_x.at[t, 0], at_x),
            lambda: (part.at[t % PARTS, 3, top], from_x.at[t, 1], at_x),
            lambda: (part.at[t % PARTS, 2, bottom], from_y.at[t, 0], at_y),
            lambda: (part.at[t % PARTS, 3, bottom], from_y.at[t, 1], at_y),
            lambda: (part.at[t % PARTS, 1, bottom], last_x.at[t], at_x),
            lambda: (part.at[t % PARTS, 2, top], last_y.at[t], at_y),
            lambda: (part.at[t % PARTS, 0], from_pair.at[t], at_pair),
            lambda: (part.at[t % PARTS, 0], from_far.at[t], at_far),
            lambda: (sums.at[t], sums.at[t], at_pair),
        )[kind]()
        return remote(t, kind, source, target, peer)

    def stage_product(t):
        lhs = left[left_of(t)]
        for column in range(0, WIDE, 256):
            block = lax.dot_general(
                lhs,
                right[right_of(t), :, pl.ds(pl.multiple_of((t % 2) * WIDE + column, 256), 256)],
                (((0,), (0,)), ((), ())),
                preferred_element_type=jnp.float32,
            ).astype(jnp.bfloat16)
            for slot in range(4):
                part[t % PARTS, slot, :, column : column + 256] = block[slot * BLOCK : (slot + 1) * BLOCK]
        for kind in (1, 3, 0, 2):
            moved(t, kind).start()

    def stage_turn(t):
        moved(t, 1).wait_recv()
        add_rows(part.at[t % PARTS, 2, top], (part.at[t % PARTS, 2, top], from_x.at[t, 1]), half)
        moved(t, 5).start()
        moved(t, 3).wait_recv()
        add_rows(part.at[t % PARTS, 1, bottom], (part.at[t % PARTS, 1, bottom], from_y.at[t, 1]), half)
        moved(t, 4).start()

    def stage_plane(t):
        moved(t, 0).wait_recv()
        moved(t, 5).wait_recv()
        add_rows(part.at[t % PARTS, 0, top], (part.at[t % PARTS, 0, top], from_x.at[t, 0], last_y.at[t]), half)
        moved(t, 2).wait_recv()
        moved(t, 4).wait_recv()
        add_rows(
            part.at[t % PARTS, 0, bottom], (part.at[t % PARTS, 0, bottom], from_y.at[t, 0], last_x.at[t]), half
        )

        @pl.when(outer)
        def _():
            moved(t, 6).start()

    def stage_pair(t):
        @pl.when(inner)
        def _():
            moved(t, 6).wait_recv()
            add_rows(part.at[t % PARTS, 0], (part.at[t % PARTS, 0], from_pair.at[t]), BLOCK)
            moved(t, 7).start()

    def stage_far(t):
        @pl.when(inner)
        def _():
            moved(t, 7).wait_recv()
            add_rows(sums.at[t], (part.at[t % PARTS, 0], from_far.at[t]), BLOCK)
            moved(t, 8).start()

    def stage_end(t):
        @pl.when(inner)
        def _():
            moved(t, 7).wait_send()
            moved(t, 8).wait_send()

        @pl.when(outer)
        def _():
            moved(t, 6).wait_send()
            moved(t, 8).wait_recv()

        for kind in range(6):
            moved(t, kind).wait_send()

        store(t, True)

    def store(t, begin):
        for low, high, target in (
            (0, 8, lambda i: out_down.at[pl.ds(pl.multiple_of(i // 2 * BLOCK, BLOCK), BLOCK), columns(i % 2)]),
            (8, 16, lambda i: out_up.at[:, columns(i)]),
            (16, 18, lambda i: out_out.at[:, columns(i)]),
            (18, 24, lambda i: out_qkv.at[:, columns(i)]),
        ):

            @pl.when((t >= low) & (t < high))
            def _(low=low, target=target):
                copy = pltpu.make_async_copy(sums.at[t], target(t - low), stored.at[t])
                copy.start() if begin else copy.wait()

    def columns(i):
        return pl.ds(pl.multiple_of(i * WIDE, WIDE), WIDE)

    def stage_stored(t):
        store(t, False)

    peers = (at_core, at_x, at_y, at_pair, at_far)

    def small_copy(j):
        return pltpu.make_async_remote_copy(
            src_ref=small_sent.at[j],
            dst_ref=small_got.at[j],
            send_sem=small_send.at[j],
            recv_sem=small_recv.at[j],
            device_id=peers[j],
            device_id_type=MESH,
        )

    stages = (stage_turn, stage_plane, stage_pair, stage_far, stage_end, stage_stored)

    def tick(t, carry):
        for when, i in new_left.items():

            @pl.when(t == when)
            def _(i=i):
                for copy in lefts[i]:
                    copy.wait()

        for when, i in new_right.items():

            @pl.when(t == when)
            def _(i=i):
                for copy in rights[i]:
                    copy.wait()

        @pl.when(t < CHUNKS)
        def _():
            stage_product(t)

        work(t)
        for lag, stage in zip(LAGS, stages):

            @pl.when((t >= lag) & (t < CHUNKS + lag))
            def _(lag=lag, stage=stage):
                stage(t - lag)

        for j in range(5):

            @pl.when(t == 23 + j)
            def _(j=j):
                small_copy(j).wait()
                total = small_sent[j] + small_got[j]
                if j < 4:
                    small_sent[j + 1] = total
                    small_copy(j + 1).start()
                else:
                    small_sums[...] = total

        return carry

    lax.fori_loop(0, CHUNKS + LAGS[-1], tick, 0)


def run_backward(lefts, grad_mlp, sources, weights, positions, documents, router, gain_one, gain_two):
    rows = grad_mlp.shape[0]
    bf16, f32, dma = jnp.bfloat16, jnp.float32, pltpu.SemaphoreType.DMA
    chunk, half_chunk = (CHUNKS, BLOCK, WIDE), (CHUNKS, BLOCK // 2, WIDE)
    held = [
        ((LEFTS, 2 * rows, 4 * BLOCK), bf16),
        ((RIGHTS, 2 * rows, FULL), bf16),
        ((PARTS, 4, BLOCK, WIDE), bf16),
        ((CHUNKS, 2, BLOCK // 2, WIDE), bf16),
        ((CHUNKS, 2, BLOCK // 2, WIDE), bf16),
        (half_chunk, bf16),
        (half_chunk, bf16),
        (chunk, bf16),
        (chunk, bf16),
        (chunk, bf16),
    ]
    held += [(source.shape, source.dtype) for source in (*sources, lefts[0])]
    held += [
        ((4, 512, FULL), bf16),
        ((2, 256, 4 * FULL), bf16),
        ((rows, FULL), f32),
        ((rows, FULL), f32),
        ((rows, FULL), bf16),
        ((8, FULL), f32),
        ((5, 8, FULL), f32),
        ((5, 8, FULL), f32),
        ((rows, 128), f32),
        ((rows, 128), jnp.int32),
        ((rows, 128), jnp.int32),
    ]
    counts = [(LEFTS, 4)] * 3 + [(RIGHTS,)] * 3 + [(CHUNKS, 9)] * 2 + [(5,)] * 2
    counts += [(CHUNKS,), (9,), (4,), (2,)]
    shapes = [(4 * BLOCK, FULL), (BLOCK, 4 * FULL), (BLOCK, 3 * FULL), (BLOCK, FULL)] + [(rows, FULL)] * 2
    return pl.pallas_call(
        reduce_kernel,
        out_shape=[jax.ShapeDtypeStruct(shape, bf16) for shape in shapes]
        + [jax.ShapeDtypeStruct((8, FULL), f32)],
        in_specs=[pl.BlockSpec(memory_space=ANY)] * 17
        + [pl.BlockSpec(memory_space=pltpu.VMEM)] * 5,
        out_specs=[pl.BlockSpec(memory_space=ANY)] * 6 + [pl.BlockSpec(memory_space=pltpu.VMEM)],
        scratch_shapes=[pltpu.VMEM(*each_one) for each_one in held] + [dma(count) for count in counts],
        compiler_params=pltpu.CompilerParams(
            collective_id=2, has_side_effects=True, vmem_limit_bytes=62 * 1024 * 1024
        ),
        name="backward_and_reduce",
    )(
        *lefts,
        grad_mlp,
        *sources,
        *weights,
        positions[None],
        documents[None],
        router[None],
        gain_one[None],
        gain_two[None],
    )


def put_rows(tokens, rows, positions):
    hit = lax.broadcasted_iota(jnp.int32, (tokens.shape[0], positions.shape[0]), 0) == positions[None]
    moved = jnp.dot(hit.astype(jnp.bfloat16), rows, preferred_element_type=jnp.float32)
    return jnp.where(jnp.any(hit, axis=1, keepdims=True), moved.astype(jnp.bfloat16), tokens)


def per_device(
    hidden, cotangent, route_pos, route_doc, w_qkv, w_out, w_up, w_down, router, gain_one, gain_two
):
    positions = route_pos[0]
    documents = route_doc[0]
    (
        full_qkv,
        full_out,
        full_up,
        full_down,
        routed,
        taken,
        normed_in,
        packed,
        attended,
        middle,
        normed_mid,
        activated,
        slope,
        grad_mlp,
        grad_branch,
        attn_out,
        gate,
    ) = run_forward(
        (w_qkv, w_out, w_up, w_down),
        8,
        hidden,
        cotangent,
        positions,
        documents,
        router,
        gain_one,
        gain_two,
    )
    *sums, rows_out, grad_rows, small_sums = run_backward(
        (activated, normed_mid, normed_in, attended),
        grad_mlp,
        (slope, attn_out, packed, middle, routed, taken, grad_branch, gate),
        (full_qkv, full_out, full_up, full_down),
        positions,
        documents,
        router,
        gain_one,
        gain_two,
    )
    output = put_rows(hidden, rows_out, positions)
    grad_hidden = put_rows(cotangent, grad_rows, positions)
    sum_down, sum_up, sum_qkv, sum_out = (total.astype(jnp.float32) for total in sums)
    return (
        output,
        grad_hidden,
        sum_qkv,
        sum_out,
        sum_up,
        sum_down,
        small_sums[0],
        small_sums[1],
        small_sums[2],
    )


def solution(mesh):
    paired = dict(mesh.shape) == {"dp": 4, "fsdp": 8}
    tokens, weights = P(("dp", "fsdp"), None), P("fsdp", None)
    return jax.shard_map(
        per_device if paired else general_device,
        mesh=mesh,
        in_specs=(tokens,) * 4 + (weights,) * 4 + (P(),) * 3,
        out_specs=(tokens,) * 2 + (weights,) * 4 + (P(),) * 3,
        check_vma=False,
    )
```
